16 devices in a mesh: dp: 2 (over y, z), ep: 8 (over x, core).
Axes of the slice: x: 4, y: 2, z: 1, core: 2. Of those that a mesh axis runs over, the one named last changes fastest.
The devices are a block of a 4x4x8 slice.
Arguments:
- hidden: bfloat16 [1024, 2048], P(('dp', 'ep')), parts along dimension 0
- positions: int32 [1024], P(('dp', 'ep')), parts along dimension 0
- expert_ids: int32 [2, 1024, 8], P(None, ('dp', 'ep')), parts along dimension 1
- k_cache: bfloat16 [2, 1024, 16, 16, 128], P(None, ('dp', 'ep')), parts along dimension 1
- v_cache: bfloat16 [2, 1024, 16, 16, 128], P(None, ('dp', 'ep')), parts along dimension 1
- w_query: bfloat16 [2, 2048, 2048], replicated
- w_key: bfloat16 [2, 2048, 2048], replicated
- w_value: bfloat16 [2, 2048, 2048], replicated
- w_out: bfloat16 [2, 2048, 2048], replicated
- attn_gain: float32 [2, 2048], replicated
- q_gain: float32 [2, 2048], replicated
- k_gain: float32 [2, 2048], replicated
- mlp_gain: float32 [2, 2048], replicated
- w_router: bfloat16 [2048, 64], replicated
- w_gate: bfloat16 [64, 2048, 1024], P('ep')
- w_up: bfloat16 [64, 2048, 1024], P('ep')
- w_down: bfloat16 [64, 1024, 2048], P('ep')
Outputs:
- output 1: bfloat16 [1024, 2048], P(('dp', 'ep')), parts along dimension 0
- output 2: bfloat16 [2, 1024, 16, 16, 128], P(None, ('dp', 'ep')), parts along dimension 1
- output 3: bfloat16 [2, 1024, 16, 16, 128], P(None, ('dp', 'ep')), parts along dimension 1
There are 2 independent parts. The reference program is written for one: setup_inputs(seed, part) draws one part's arguments, and reference() takes and returns one part's arrays. A program takes and returns all parts, laid end to end along the dimension named above; an argument that names none is the same for every part.
All inputs are finite; a program needn't handle non-finite values.
Results may differ from the reference program's by a relative error of at most 0.02.
Values are sent between devices in bfloat16 or wider.
A program may use at most 768 MiB of HBM per device.

```python
import jax
import jax.numpy as jnp
from jax import lax

SEQ_COUNT = 512
CACHE_LEN = 16
MODEL_DIM = 2048
NUM_HEADS = 16
KV_HEADS = 16
HEAD_DIM = 128
NUM_EXPERTS = 64
TOP_K = 8
FFN_DIM = 1024
EP_GROUPS = 8
NUM_LAYERS = 2

LOCAL_SEQS = SEQ_COUNT // EP_GROUPS
CAPACITY = 2 * LOCAL_SEQS * TOP_K // NUM_EXPERTS
WINDOWS = NUM_EXPERTS // TOP_K
Q_WIDTH = NUM_HEADS * HEAD_DIM
KV_WIDTH = KV_HEADS * HEAD_DIM
RMS_EPS = 1e-5
ROPE_BASE = 10000.0


def block_routes(rng_key):
    key_rows, key_perm = jax.random.split(rng_key)
    spread = jnp.arange(LOCAL_SEQS - CAPACITY, dtype=jnp.int32) % (WINDOWS - 1) + 1
    window_list = jnp.concatenate([jnp.zeros((CAPACITY,), jnp.int32), spread])
    windows = window_list[jax.random.permutation(key_rows, LOCAL_SEQS)]
    expert_perm = jax.random.permutation(key_perm, NUM_EXPERTS).astype(jnp.int32)
    slot_ids = windows[:, None] * TOP_K + jnp.arange(TOP_K, dtype=jnp.int32)[None, :]
    return expert_perm[slot_ids]


def draw_routes(rng_key):
    layer_keys = jax.random.split(rng_key, NUM_LAYERS * EP_GROUPS)
    routes = jax.vmap(block_routes)(layer_keys)
    return routes.reshape(NUM_LAYERS, SEQ_COUNT, TOP_K)


def draw_positions(rng_key):
    key_len, key_top = jax.random.split(rng_key)
    positions = jax.random.randint(key_len, (SEQ_COUNT,), 0, CACHE_LEN, dtype=jnp.int32)
    longest = jax.random.randint(key_top, (), 0, SEQ_COUNT)
    return positions.at[longest].set(CACHE_LEN - 1)


def setup_inputs(seed: int = 0, part: int = 0) -> dict:
    part_keys = jax.random.split(jax.random.fold_in(jax.random.key(seed + 1), part), 5)
    shared = jax.random.split(jax.random.key(seed), 12)

    def draw_normal(rng_key, shape, scale):
        return (jax.random.normal(rng_key, shape, jnp.float32) * scale).astype(jnp.bfloat16)

    def draw_gain(rng_key, shape):
        return 1.0 + 0.3 * jax.random.normal(rng_key, shape, jnp.float32)

    cache_shape = (NUM_LAYERS, SEQ_COUNT, CACHE_LEN, KV_HEADS, HEAD_DIM)
    return dict(
        hidden=draw_normal(part_keys[0], (SEQ_COUNT, MODEL_DIM), 1.0),
        positions=draw_positions(part_keys[1]),
        expert_ids=draw_routes(part_keys[2]),
        k_cache=draw_normal(part_keys[3], cache_shape, 1.0),
        v_cache=draw_normal(part_keys[4], cache_shape, 1.0),
        w_query=draw_normal(shared[0], (NUM_LAYERS, MODEL_DIM, Q_WIDTH), MODEL_DIM ** -0.5),
        w_key=draw_normal(shared[1], (NUM_LAYERS, MODEL_DIM, KV_WIDTH), MODEL_DIM ** -0.5),
        w_value=draw_normal(shared[2], (NUM_LAYERS, MODEL_DIM, KV_WIDTH), MODEL_DIM ** -0.5),
        w_out=draw_normal(shared[3], (NUM_LAYERS, Q_WIDTH, MODEL_DIM), 2.0 * Q_WIDTH ** -0.5),
        attn_gain=draw_gain(shared[4], (NUM_LAYERS, MODEL_DIM)),
        q_gain=draw_gain(shared[5], (NUM_LAYERS, Q_WIDTH)),
        k_gain=draw_gain(shared[6], (NUM_LAYERS, KV_WIDTH)),
        mlp_gain=draw_gain(shared[7], (NUM_LAYERS, MODEL_DIM)),
        w_router=draw_normal(shared[8], (MODEL_DIM, NUM_EXPERTS), MODEL_DIM ** -0.5),
        w_gate=draw_normal(shared[9], (NUM_EXPERTS, MODEL_DIM, FFN_DIM), MODEL_DIM ** -0.5),
        w_up=draw_normal(shared[10], (NUM_EXPERTS, MODEL_DIM, FFN_DIM), MODEL_DIM ** -0.5),
        w_down=draw_normal(shared[11], (NUM_EXPERTS, FFN_DIM, MODEL_DIM), NUM_EXPERTS * TOP_K ** -0.5 * FFN_DIM ** -0.5),
    )


def rms_norm(values, gain_vec):
    values = values.astype(jnp.float32)
    inv_rms = lax.rsqrt(jnp.mean(values * values, axis=-1, keepdims=True) + RMS_EPS)
    return values * inv_rms * gain_vec.astype(jnp.float32)


def rope_rotate(values, positions):
    half_dim = values.shape[-1] // 2
    frequencies = ROPE_BASE ** (-jnp.arange(half_dim, dtype=jnp.float32) / half_dim)
    angles = positions.astype(jnp.float32)[:, None] * frequencies[None, :]
    angles = angles.reshape((angles.shape[0],) + (1,) * (values.ndim - 2) + (half_dim,))
    cosines = jnp.cos(angles)
    sines = jnp.sin(angles)
    first_half = values[..., :half_dim]
    second_half = values[..., half_dim:]
    return jnp.concatenate([first_half * cosines - second_half * sines, second_half * cosines + first_half * sines], axis=-1)


def attention_layer(hidden, positions, k_layer, v_layer, w_query, w_key, w_value, w_out, attn_gain, q_gain, k_gain):
    head_group = NUM_HEADS // KV_HEADS
    normed = rms_norm(hidden, attn_gain).astype(jnp.bfloat16)
    q_heads = rms_norm(jnp.dot(normed, w_query, preferred_element_type=jnp.float32), q_gain)
    key_row = rms_norm(jnp.dot(normed, w_key, preferred_element_type=jnp.float32), k_gain)
    value_row = jnp.dot(normed, w_value, preferred_element_type=jnp.float32).astype(jnp.bfloat16)
    value_row = value_row.reshape(SEQ_COUNT, KV_HEADS, HEAD_DIM)
    q_heads = rope_rotate(q_heads.reshape(SEQ_COUNT, KV_HEADS, head_group, HEAD_DIM), positions).astype(jnp.bfloat16)
    key_row = rope_rotate(key_row.reshape(SEQ_COUNT, KV_HEADS, HEAD_DIM), positions).astype(jnp.bfloat16)
    hit_mask = (jnp.arange(CACHE_LEN)[None, :] == positions[:, None])[:, :, None, None]
    k_layer = jnp.where(hit_mask, key_row[:, None], k_layer)
    v_layer = jnp.where(hit_mask, value_row[:, None], v_layer)
    scores = jnp.einsum('bkgd,bskd->bkgs', q_heads.astype(jnp.float32), k_layer.astype(jnp.float32)) * HEAD_DIM ** -0.5
    valid_mask = (jnp.arange(CACHE_LEN)[None, :] <= positions[:, None])[:, None, None, :]
    scores = jnp.where(valid_mask, scores, -1e30)
    prob_vals = jax.nn.softmax(scores, axis=-1).astype(jnp.bfloat16)
    mixed_out = jnp.einsum('bkgs,bskd->bkgd', prob_vals.astype(jnp.float32), v_layer.astype(jnp.float32))
    mixed_out = mixed_out.astype(jnp.bfloat16).reshape(SEQ_COUNT, Q_WIDTH)
    hidden = (hidden.astype(jnp.float32) + jnp.dot(mixed_out, w_out, preferred_element_type=jnp.float32)).astype(jnp.bfloat16)
    return hidden, k_layer, v_layer


def moe_layer(hidden, routes, mlp_gain, w_router, w_gate, w_up, w_down):
    normed = rms_norm(hidden, mlp_gain).astype(jnp.bfloat16)
    router_prob = jax.nn.softmax(jnp.dot(normed, w_router, preferred_element_type=jnp.float32), axis=-1)
    gate_vals = jnp.take_along_axis(router_prob, routes, axis=1)
    flat_ids = routes.reshape(-1)
    sort_order = jnp.argsort(flat_ids, stable=True)
    counts = jnp.sum(flat_ids[:, None] == jnp.arange(NUM_EXPERTS)[None, :], axis=0, dtype=jnp.int32)
    starts = jnp.cumsum(counts) - counts
    per_expert = EP_GROUPS * CAPACITY
    padded = jnp.concatenate([sort_order, jnp.zeros((per_expert,), sort_order.dtype)])

    def expert_rows(item_pair):
        expert, start_at = item_pair
        copies = lax.dynamic_slice(padded, (start_at,), (per_expert,))
        token_rows = normed[copies // TOP_K]
        gate_act = jnp.dot(token_rows, w_gate[expert], preferred_element_type=jnp.float32)
        up_act = jnp.dot(token_rows, w_up[expert], preferred_element_type=jnp.float32)
        hidden_act = (jax.nn.silu(gate_act) * up_act).astype(jnp.bfloat16)
        return jnp.dot(hidden_act, w_down[expert], preferred_element_type=jnp.float32).astype(jnp.bfloat16)

    outputs = lax.map(expert_rows, (jnp.arange(NUM_EXPERTS), starts))
    copy_rank = jnp.argsort(sort_order, stable=True)
    within = copy_rank - starts[flat_ids]
    picked = outputs[flat_ids, within].reshape(SEQ_COUNT, TOP_K, MODEL_DIM)
    moe_out = jnp.sum(gate_vals[:, :, None] * picked.astype(jnp.float32), axis=1)
    return (hidden.astype(jnp.float32) + moe_out).astype(jnp.bfloat16)


def reference(hidden, positions, expert_ids, k_cache, v_cache, w_query, w_key, w_value, w_out, attn_gain, q_gain, k_gain, mlp_gain, w_router, w_gate, w_up, w_down):
    k_layers = []
    v_layers = []
    for layer_idx in range(NUM_LAYERS):
        hidden, k_layer, v_layer = attention_layer(hidden, positions, k_cache[layer_idx], v_cache[layer_idx], w_query[layer_idx], w_key[layer_idx], w_value[layer_idx], w_out[layer_idx], attn_gain[layer_idx], q_gain[layer_idx], k_gain[layer_idx])
        k_layers.append(k_layer)
        v_layers.append(v_layer)
        hidden = moe_layer(hidden, expert_ids[layer_idx], mlp_gain[layer_idx], w_router, w_gate, w_up, w_down)
    return hidden, jnp.stack(k_layers), jnp.stack(v_layers)
```

```python
import functools

import jax
import jax.numpy as jnp
from jax import lax
from jax.experimental import pallas as pl
from jax.experimental.pallas import tpu as pltpu
from jax.sharding import PartitionSpec as P

RMS_EPS = 1e-5
ROPE_BASE = 10000.0
CAP_FACTOR = 2
MESH = pl.DeviceIdType.MESH
AG_PARTS = 2
RS_CHUNKS = 4
UNIT = 1024
RING = 20


def rms_norm(values, gain_vec):
    values = values.astype(jnp.float32)
    inv_rms = lax.rsqrt(jnp.mean(values * values, axis=-1, keepdims=True) + RMS_EPS)
    return values * inv_rms * gain_vec.astype(jnp.float32)


def rope_rotate(values, positions):
    half_dim = values.shape[-1] // 2
    frequencies = ROPE_BASE ** (-jnp.arange(half_dim, dtype=jnp.float32) / half_dim)
    angles = positions.astype(jnp.float32)[:, None] * frequencies[None, :]
    angles = angles.reshape((angles.shape[0],) + (1,) * (values.ndim - 2) + (half_dim,))
    cosines = jnp.cos(angles)
    sines = jnp.sin(angles)
    first_half = values[..., :half_dim]
    second_half = values[..., half_dim:]
    return jnp.concatenate([first_half * cosines - second_half * sines, second_half * cosines + first_half * sines], axis=-1)


def attention_local(hidden, positions, k_layer, v_layer, w_query, w_key, w_value, w_out, attn_gain, q_gain, k_gain):
    seq_rows = hidden.shape[0]
    cache_len, kv_heads, head_dim = k_layer.shape[1:]
    head_group = w_query.shape[1] // head_dim // kv_heads
    normed = rms_norm(hidden, attn_gain).astype(jnp.bfloat16)
    q_heads = rms_norm(jnp.dot(normed, w_query, preferred_element_type=jnp.float32), q_gain)
    key_row = rms_norm(jnp.dot(normed, w_key, preferred_element_type=jnp.float32), k_gain)
    value_row = jnp.dot(normed, w_value, preferred_element_type=jnp.float32).astype(jnp.bfloat16)
    value_row = value_row.reshape(seq_rows, kv_heads, head_dim)
    q_heads = rope_rotate(q_heads.reshape(seq_rows, kv_heads, head_group, head_dim), positions).astype(jnp.bfloat16)
    key_row = rope_rotate(key_row.reshape(seq_rows, kv_heads, head_dim), positions).astype(jnp.bfloat16)
    score_scale = head_dim ** -0.5
    past_scores = jnp.einsum('bkgd,bskd->bkgs', q_heads, k_layer, preferred_element_type=jnp.float32) * score_scale
    before = (jnp.arange(cache_len)[None, :] < positions[:, None])[:, None, None, :]
    past_scores = jnp.where(before, past_scores, -1e30)
    new_score = jnp.einsum('clhe,cle->clh', q_heads, key_row, preferred_element_type=jnp.float32)[..., None] * score_scale
    peak_score = jnp.maximum(jnp.max(past_scores, axis=-1, keepdims=True), new_score)
    past_exp = jnp.exp(past_scores - peak_score)
    new_exp = jnp.exp(new_score - peak_score)
    prob_sum = jnp.sum(past_exp, axis=-1, keepdims=True) + new_exp
    past_prob = (past_exp / prob_sum).astype(jnp.bfloat16)
    new_prob = (new_exp / prob_sum).astype(jnp.bfloat16)
    mixed_out = jnp.einsum('bkgs,bskd->bkgd', past_prob, v_layer, preferred_element_type=jnp.float32)
    mixed_out = mixed_out + new_prob.astype(jnp.float32) * value_row.astype(jnp.float32)[:, :, None, :]
    mixed_out = mixed_out.astype(jnp.bfloat16).reshape(seq_rows, kv_heads * head_group * head_dim)
    hidden = (hidden.astype(jnp.float32) + jnp.dot(mixed_out, w_out, preferred_element_type=jnp.float32)).astype(jnp.bfloat16)
    return hidden, key_row, value_row


def moe_kernel(groups, x_ref, routes_ref, gain_ref, wr_ref, wg, wu, wd, out_ref, ring, rows, xg, act, ys, smat, meta, meta_in, part, dbuf, tbuf, f1, f2, ring_sem, ag_send, ag_recv, meta_send, meta_recv, rs_send, rs_recv):
    seqs, model = x_ref.shape
    local_experts = wg.shape[0]
    experts = wr_ref.shape[1]
    ffn = wg.shape[2]
    slots = xg.shape[1] // groups
    chips = groups // 2
    me = lax.axis_index('ep')
    chip, core = me // 2, me % 2
    step = 1 - 2 * core
    partner = chip * 2 + 1 - core

    def device(offset, core_idx):
        return ((chip + offset + chips) % chips) * 2 + core_idx

    long_dev, short_dev, far_dev = device(step, core), device(-step, core), device(2 * step, core)
    gate_units = 2 * model // UNIT
    down_units = model // UNIT
    total_gate = gate_units * local_experts

    def gate_copy(expert, j):
        weights = wg if j < gate_units // 2 else wu
        slot = (expert * gate_units + j) % RING
        return pltpu.make_async_copy(weights.at[expert, pl.ds((j % (gate_units // 2)) * UNIT, UNIT), :], ring.at[slot], ring_sem.at[slot])

    def down_slot(unit):
        return (total_gate + unit) % RING

    def down_copy(unit):
        half, expert = unit // local_experts, unit % local_experts
        slot = down_slot(unit)
        return pltpu.make_async_copy(wd.at[expert, :, pl.ds(pl.multiple_of(half * UNIT, UNIT), UNIT)], ring.at[slot], ring_sem.at[slot])

    ahead = RING // gate_units
    for expert in range(ahead):
        for j in range(gate_units):
            gate_copy(expert, j).start()

    barrier = pltpu.get_barrier_semaphore()
    for j in range(1, groups):
        pl.semaphore_signal(barrier, inc=1, device_id={'ep': (me + j) % groups}, device_id_type=MESH)

    values = x_ref[...].astype(jnp.float32)
    inv_rms = lax.rsqrt(jnp.mean(values * values, axis=-1, keepdims=True) + RMS_EPS)
    normed = (values * inv_rms * gain_ref[...]).astype(jnp.bfloat16)
    rows[me] = normed
    pl.semaphore_wait(barrier, groups - 1)

    part_rows = seqs // AG_PARTS

    def rows_copy(role, source, peer, q):
        ref = rows.at[source, pl.ds(q * part_rows, part_rows), :]
        return pltpu.make_async_remote_copy(src_ref=ref, dst_ref=ref, send_sem=ag_send.at[role, q], recv_sem=ag_recv.at[role, q], device_id={'ep': peer}, device_id_type=MESH)

    plan = [(me, partner), (me, long_dev), (me, short_dev), (short_dev, long_dev), (short_dev, partner), (long_dev, partner), (far_dev, partner)]
    copies = [[rows_copy(role, source, peer, q) for q in range(AG_PARTS)] for role, (source, peer) in enumerate(plan)]
    for q in range(AG_PARTS):
        for role in (1, 2, 0):
            copies[role][q].start()

    logits = jnp.dot(normed, wr_ref[...], preferred_element_type=jnp.float32)
    shifted = jnp.exp(logits - jnp.max(logits, axis=-1, keepdims=True))
    prob = shifted / jnp.sum(shifted, axis=-1, keepdims=True)
    expert_iota = lax.broadcasted_iota(jnp.int32, (seqs, experts), 1)
    routes = routes_ref[...]
    chosen = expert_iota == routes[:, 0:1]
    for j in range(1, routes.shape[1]):
        chosen = chosen | (expert_iota == routes[:, j:j + 1])
    row_iota = lax.broadcasted_iota(jnp.int32, (seqs, seqs), 0)
    col_iota = lax.broadcasted_iota(jnp.int32, (seqs, seqs), 1)
    lower = jnp.where(col_iota < row_iota, 1.0, 0.0).astype(jnp.bfloat16)
    ranks = jnp.dot(lower, jnp.where(chosen, 1.0, 0.0).astype(jnp.bfloat16), preferred_element_type=jnp.float32)
    ranks = jnp.where(chosen, ranks, -1.0)
    gates = jnp.where(chosen, prob, 0.0)
    both = jnp.concatenate([jnp.concatenate([ranks, gates], axis=1), jnp.zeros((2 * experts - seqs, 2 * experts), jnp.float32)], axis=0)
    both_t = both.T
    meta[:, :2 * experts] = both_t[:experts]
    meta[:, 2 * experts:] = both_t[experts:]

    def meta_copy(j):
        peer = (me + j) % groups
        return pltpu.make_async_remote_copy(src_ref=meta.at[pl.ds(pl.multiple_of(peer * local_experts, local_experts), local_experts), :], dst_ref=meta_in.at[me], send_sem=meta_send.at[j], recv_sem=meta_recv.at[j], device_id={'ep': peer}, device_id_type=MESH)

    meta_copies = [meta_copy(j) for j in range(1, groups)]
    meta_in[me] = meta[pl.ds(pl.multiple_of(me * local_experts, local_experts), local_experts), :]
    for copy in meta_copies:
        copy.start()

    def gather(source):
        info = meta_in[source]
        rank = info[:, :2 * experts].reshape(local_experts, 1, 2 * experts)
        gate = info[:, 2 * experts:].reshape(local_experts, 1, 2 * experts)
        place = lax.broadcasted_iota(jnp.int32, (local_experts, slots, 2 * experts), 1).astype(jnp.float32)
        hit = jnp.broadcast_to(rank, place.shape) == place
        total = local_experts * slots
        onehot = jnp.where(hit, 1.0, 0.0).reshape(total, 2 * experts)[:, :seqs].astype(jnp.bfloat16)
        taken = jnp.dot(onehot, rows[source], preferred_element_type=jnp.float32).astype(jnp.bfloat16)
        at = pl.ds(pl.multiple_of(source * slots, slots), slots)
        for e in range(local_experts):
            xg[e, at, :] = taken[e * slots:(e + 1) * slots]
        weight = jnp.where(hit, jnp.broadcast_to(gate, place.shape), 0.0).reshape(total, 2 * experts).T[:seqs]
        first = weight.astype(jnp.bfloat16)
        rest = weight - first.astype(jnp.float32)
        second = rest.astype(jnp.bfloat16)
        third = (rest - second.astype(jnp.float32)).astype(jnp.bfloat16)
        smat[source, pl.ds(0, seqs), :] = first
        smat[source, pl.ds(seqs, seqs), :] = second
        smat[source, pl.ds(2 * seqs, seqs), :] = third

    gather(me)
    for q in range(AG_PARTS):
        copies[1][q].wait_recv()
        copies[3][q].start()
        copies[4][q].start()
        copies[2][q].wait_recv()
        copies[5][q].start()
    for copy in meta_copies:
        copy.wait_recv()
    for q in range(AG_PARTS):
        copies[0][q].wait_recv()
    gather(partner)
    gather(short_dev)
    gather(long_dev)
    for role in (4, 5):
        for q in range(AG_PARTS):
            copies[role][q].wait_recv()
    gather(device(step, 1 - core))
    gather(device(-step, 1 - core))
    for q in range(AG_PARTS):
        copies[3][q].wait_recv()
        copies[6][q].start()
    gather(far_dev)
    for q in range(AG_PARTS):
        copies[6][q].wait_recv()
    gather(device(2 * step, 1 - core))

    def expert_body(e, carry):
        def product(first):
            total = None
            for j in range(gate_units // 2):
                slot = (e * gate_units + first + j) % RING
                gate_copy(e, first + j).wait()
                term = jnp.dot(xg[e, :, pl.ds(j * UNIT, UNIT)], ring[slot], preferred_element_type=jnp.float32)
                total = term if total is None else total + term
            return total

        gate_act = product(0)
        up_act = product(gate_units // 2)
        act[e] = (jax.nn.silu(gate_act) * up_act).astype(jnp.bfloat16)

        @pl.when(e + ahead < local_experts)
        def _():
            for j in range(gate_units):
                gate_copy(e + ahead, j).start()

        first_unit = (e + ahead - local_experts) * gate_units

        @pl.when((first_unit >= 0) & (first_unit < down_units * local_experts))
        def _():
            for j in range(gate_units):
                down_copy(first_unit + j).start()

        return carry

    lax.fori_loop(0, local_experts, expert_body, 0)

    width = model // RS_CHUNKS
    per_unit = UNIT // width

    def rs_copy(role, k, source, target, peer):
        return pltpu.make_async_remote_copy(src_ref=source, dst_ref=target, send_sem=rs_send.at[role, k], recv_sem=rs_recv.at[role, k], device_id={'ep': peer}, device_id_type=MESH)

    far_chip, long_chip, short_chip = far_dev // 2, long_dev // 2, short_dev // 2

    def pair_copy(k):
        return rs_copy(0, k, part.at[k, 1 - core], dbuf.at[k], partner)

    def far_copy(k):
        return rs_copy(1, k, part.at[k, core, far_chip], tbuf.at[k], long_dev)

    def short_copy(k):
        return rs_copy(2, k, part.at[k, core, short_chip], f1.at[k], short_dev)

    def long_copy(k):
        return rs_copy(3, k, part.at[k, core, long_chip], f2.at[k], long_dev)

    def compute_chunk(k):
        half = k // per_unit
        column = (k % per_unit) * width

        def down_body(i, carry):
            for u in range(4):
                e = i * 4 + u
                unit = half * local_experts + e
                slot = down_slot(unit)
                if k % per_unit == 0:
                    down_copy(unit).wait()
                out = jnp.dot(act[e], ring[slot, :, pl.ds(column, width)], preferred_element_type=jnp.float32).astype(jnp.bfloat16)
                at = pl.ds(pl.multiple_of(e * slots, slots), slots)
                for b in range(groups):
                    ys[b, at, :] = out[b * slots:(b + 1) * slots]
            return carry

        lax.fori_loop(0, local_experts // 4, down_body, 0)
        for b in range(groups):
            sums = jnp.dot(smat[b], ys[b], preferred_element_type=jnp.float32)
            part[k, b % 2, b // 2] = sums[:seqs] + sums[seqs:2 * seqs] + sums[2 * seqs:]

    def pair_sum(k):
        pair_copy(k).wait_recv()
        part[k, core] = part[k, core] + dbuf[k]
        far_copy(k).start()
        short_copy(k).start()

    def forward(k):
        far_copy(k).wait_recv()
        part[k, core, long_chip] = part[k, core, long_chip] + tbuf[k]
        long_copy(k).start()

    def finish(k):
        short_copy(k).wait_recv()
        long_copy(k).wait_recv()
        moe_out = part[k, core, chip] + f1[k] + f2[k]
        at = pl.ds(k * width, width)
        out_ref[:, at] = (x_ref[:, at].astype(jnp.float32) + moe_out).astype(jnp.bfloat16)

    for k in range(RS_CHUNKS):
        compute_chunk(k)
        pair_copy(k).start()
        if k >= 1:
            pair_sum(k - 1)
        if k >= 2:
            forward(k - 2)
    pair_sum(RS_CHUNKS - 1)
    for k in range(RS_CHUNKS - 2, RS_CHUNKS):
        forward(k)
    for k in range(RS_CHUNKS):
        finish(k)
    for group in copies:
        for copy in group:
            copy.wait_send()
    for copy in meta_copies:
        copy.wait_send()
    for k in range(RS_CHUNKS):
        for make in (pair_copy, far_copy, short_copy, long_copy):
            make(k).wait_send()


def moe_local(hidden, routes, mlp_gain, w_router, w_gate, w_up, w_down, groups, layer):
    seqs, model = hidden.shape
    experts = w_router.shape[1]
    local_experts, _, ffn = w_gate.shape
    slots = CAP_FACTOR * seqs * routes.shape[1] // experts
    chips = groups // 2
    width = model // RS_CHUNKS
    vmem = pl.BlockSpec(memory_space=pltpu.VMEM)
    hbm = pl.BlockSpec(memory_space=pl.ANY)
    return pl.pallas_call(
        functools.partial(moe_kernel, groups),
        out_shape=jax.ShapeDtypeStruct((seqs, model), jnp.bfloat16),
        in_specs=[vmem, vmem, vmem, vmem, hbm, hbm, hbm],
        out_specs=vmem,
        scratch_shapes=[
            pltpu.VMEM((RING, UNIT, ffn), jnp.bfloat16),
            pltpu.VMEM((groups, seqs, model), jnp.bfloat16),
            pltpu.VMEM((local_experts, groups * slots, model), jnp.bfloat16),
            pltpu.VMEM((local_experts, groups * slots, ffn), jnp.bfloat16),
            pltpu.VMEM((groups, local_experts * slots, width), jnp.bfloat16),
            pltpu.VMEM((groups, 3 * seqs, local_experts * slots), jnp.bfloat16),
            pltpu.VMEM((experts, 4 * experts), jnp.float32),
            pltpu.VMEM((groups, local_experts, 4 * experts), jnp.float32),
            pltpu.VMEM((RS_CHUNKS, 2, chips, seqs, width), jnp.float32),
            pltpu.VMEM((RS_CHUNKS, chips, seqs, width), jnp.float32),
            pltpu.VMEM((RS_CHUNKS, seqs, width), jnp.float32),
            pltpu.VMEM((RS_CHUNKS, seqs, width), jnp.float32),
            pltpu.VMEM((RS_CHUNKS, seqs, width), jnp.float32),
            pltpu.SemaphoreType.DMA((RING,)),
            pltpu.SemaphoreType.DMA((7, AG_PARTS)),
            pltpu.SemaphoreType.DMA((7, AG_PARTS)),
            pltpu.SemaphoreType.DMA((groups,)),
            pltpu.SemaphoreType.DMA((groups,)),
            pltpu.SemaphoreType.DMA((4, RS_CHUNKS)),
            pltpu.SemaphoreType.DMA((4, RS_CHUNKS)),
        ],
        compiler_params=pltpu.CompilerParams(collective_id=layer, has_side_effects=True, vmem_limit_bytes=67043328),
        name='moe_layer',
    )(hidden, routes, mlp_gain.reshape(1, model), w_router, w_gate, w_up, w_down)


def solution(mesh):
    groups = mesh.shape['ep']
    batch_axes = ('dp', 'ep')

    def device_step(hidden, positions, expert_ids, k_cache, v_cache, w_query, w_key, w_value, w_out, attn_gain, q_gain, k_gain, mlp_gain, w_router, w_gate, w_up, w_down):
        key_rows = []
        value_rows = []
        for layer_idx in range(expert_ids.shape[0]):
            hidden, key_row, value_row = attention_local(hidden, positions, k_cache[layer_idx], v_cache[layer_idx], w_query[layer_idx], w_key[layer_idx], w_value[layer_idx], w_out[layer_idx], attn_gain[layer_idx], q_gain[layer_idx], k_gain[layer_idx])
            key_rows.append(key_row)
            value_rows.append(value_row)
            hidden = moe_local(hidden, expert_ids[layer_idx], mlp_gain[layer_idx], w_router, w_gate, w_up, w_down, groups, layer_idx)
        hit_mask = (jnp.arange(k_cache.shape[2])[None, :] == positions[:, None])[None, :, :, None, None]
        k_new = jnp.where(hit_mask, jnp.stack(key_rows)[:, :, None], k_cache)
        v_new = jnp.where(hit_mask, jnp.stack(value_rows)[:, :, None], v_cache)
        return hidden, k_new, v_new

    row_spec = P(batch_axes, None)
    cache_spec = P(None, batch_axes, None, None, None)
    full_spec = P()
    expert_spec = P('ep', None, None)
    in_specs = (row_spec, P(batch_axes), P(None, batch_axes, None), cache_spec, cache_spec, full_spec, full_spec, full_spec, full_spec, full_spec, full_spec, full_spec, full_spec, full_spec, expert_spec, expert_spec, expert_spec)
    return jax.shard_map(device_step, mesh=mesh, in_specs=in_specs, out_specs=(row_spec, cache_spec, cache_spec), check_vma=False)
```

```python
import functools

import jax
import jax.numpy as jnp
from jax import lax
from jax.experimental import pallas as pl
from jax.experimental.pallas import tpu as pltpu
from jax.sharding import PartitionSpec as P

RMS_EPS = 1e-5
ROPE_BASE = 10000.0
CAP_FACTOR = 2
MESH = pl.DeviceIdType.MESH
AG_PARTS = 2
RS_CHUNKS = 4
UNIT = 1024
RING = 20
COLS = 512
CACHE_BLOCKS = 4
ATTEND_UNROLL = 4


def rms_norm(values, gain_vec):
    values = values.astype(jnp.float32)
    inv_rms = lax.rsqrt(jnp.mean(values * values, axis=-1, keepdims=True) + RMS_EPS)
    return values * inv_rms * gain_vec.astype(jnp.float32)


def rope_tables(positions, head_dim):
    half_dim = head_dim // 2
    frequencies = ROPE_BASE ** (-jnp.arange(half_dim, dtype=jnp.float32) / half_dim)
    angles = positions.astype(jnp.float32)[:, None] * frequencies[None, :]
    cosines, sines = jnp.cos(angles), jnp.sin(angles)
    return jnp.concatenate([cosines, cosines], axis=1), jnp.concatenate([-sines, sines], axis=1)


def attention_kernel(layer, aliased, pos_ref, x_ref, cos_ref, sin_ref, attn_gain, q_gain, k_gain, wq, wk, wv, wo, k_in, v_in, *rest):
    rest = rest[2:] if aliased else rest
    x_out, k_out, v_out, wbuf, kbuf, vbuf, proj, q_rows, k_rows, v_rows, mixed_rows, mixed, w_sem, in_sem, out_sem = rest
    seqs, model = x_ref.shape
    cache_len, heads, head_dim = kbuf.shape[1:]
    cols = wbuf.shape[2]
    chunks = model // cols
    block = seqs // CACHE_BLOCKS

    def weight_copy(index):
        weights = (wq, wk, wv, wo)[index // chunks]
        return pltpu.make_async_copy(weights.at[layer, :, pl.ds((index % chunks) * cols, cols)], wbuf.at[index], w_sem.at[index])

    def cache_in(kind, i):
        source, target = ((k_in, kbuf), (v_in, vbuf))[kind]
        part = pl.ds(i * block, block)
        return pltpu.make_async_copy(source.at[layer, part], target.at[part], in_sem.at[kind, i])

    def cache_out(kind, i):
        source, target = ((kbuf, k_out), (vbuf, v_out))[kind]
        part = pl.ds(i * block, block)
        return pltpu.make_async_copy(source.at[part], target.at[layer, part], out_sem.at[kind, i])

    for index in range(3 * chunks):
        weight_copy(index).start()
    for i in range(CACHE_BLOCKS):
        for kind in range(2):
            cache_in(kind, i).start()
    for index in range(3 * chunks, 4 * chunks):
        weight_copy(index).start()

    normed = rms_norm(x_ref[...], attn_gain[layer:layer + 1, :]).astype(jnp.bfloat16)

    def project(kind):
        for c in range(chunks):
            weight_copy(kind * chunks + c).wait()
            proj[kind, :, c * cols:(c + 1) * cols] = jnp.dot(normed, wbuf[kind * chunks + c], preferred_element_type=jnp.float32)

    def rotate(kind, gain, target):
        values = proj[kind]
        inv_rms = lax.rsqrt(jnp.mean(values * values, axis=-1, keepdims=True) + RMS_EPS)
        cosines, sines = cos_ref[...], sin_ref[...]
        for h in range(heads):
            at = slice(h * head_dim, (h + 1) * head_dim)
            head = proj[kind, :, at] * inv_rms * gain[layer:layer + 1, at]
            turned = head * cosines + pltpu.roll(head, head_dim // 2, 1) * sines
            target[pl.ds(h, seqs, stride=heads), :] = turned.astype(jnp.bfloat16).astype(jnp.float32)

    project(0)
    rotate(0, q_gain, q_rows)
    project(1)
    rotate(1, k_gain, k_rows)
    project(2)
    for h in range(heads):
        v_rows[pl.ds(h, seqs, stride=heads), :] = proj[2, :, h * head_dim:(h + 1) * head_dim]

    scale = head_dim ** -0.5
    row_iota = lax.broadcasted_iota(jnp.int32, (cache_len, heads, 1), 0)

    def attend(b):
        position = pos_ref[b]
        at = pl.ds(pl.multiple_of(b * heads, heads), heads)
        kbuf[b, position] = k_rows[at, :].astype(jnp.bfloat16)
        vbuf[b, position] = v_rows[at, :].astype(jnp.bfloat16)
        scores = jnp.sum(kbuf[b].astype(jnp.float32) * q_rows[at, :][None], axis=-1, keepdims=True) * scale
        scores = jnp.where(row_iota <= position, scores, -1e30)
        weights = jnp.exp(scores - jnp.max(scores, axis=0, keepdims=True))
        prob = (weights / jnp.sum(weights, axis=0, keepdims=True)).astype(jnp.bfloat16).astype(jnp.float32)
        mixed_rows[at, :] = jnp.sum(prob * vbuf[b].astype(jnp.float32), axis=0)

    for i in range(CACHE_BLOCKS):
        for kind in range(2):
            cache_in(kind, i).wait()

        def body(step, carry):
            for u in range(ATTEND_UNROLL):
                attend(i * block + step * ATTEND_UNROLL + u)
            return carry

        lax.fori_loop(0, block // ATTEND_UNROLL, body, 0)
        for kind in range(2):
            cache_out(kind, i).start()

    for h in range(heads):
        mixed[:, h * head_dim:(h + 1) * head_dim] = mixed_rows[pl.ds(h, seqs, stride=heads), :].astype(jnp.bfloat16)
    for c in range(chunks):
        weight_copy(3 * chunks + c).wait()
        at = slice(c * cols, (c + 1) * cols)
        added = jnp.dot(mixed[...], wbuf[3 * chunks + c], preferred_element_type=jnp.float32)
        x_out[:, at] = (x_ref[:, at].astype(jnp.float32) + added).astype(jnp.bfloat16)
    for i in range(CACHE_BLOCKS):
        for kind in range(2):
            cache_out(kind, i).wait()


def attention_local(layer, hidden, positions, cosines, sines, attn_gain, q_gain, k_gain, w_query, w_key, w_value, w_out, k_cache, v_cache, k_new, v_new):
    seqs, model = hidden.shape
    cache_shape = k_cache.shape[1:]
    heads, head_dim = cache_shape[2:]
    vmem = pl.BlockSpec(memory_space=pltpu.VMEM)
    smem = pl.BlockSpec(memory_space=pltpu.SMEM)
    hbm = pl.BlockSpec(memory_space=pl.ANY)
    operands = [positions, hidden, cosines, sines, attn_gain, q_gain, k_gain, w_query, w_key, w_value, w_out, k_cache, v_cache]
    specs = [smem] + [vmem] * 6 + [hbm] * 6
    aliases = {}
    if k_new is not None:
        aliases = {len(operands): 1, len(operands) + 1: 2}
        operands += [k_new, v_new]
        specs += [hbm, hbm]
    chunks = model // COLS
    return pl.pallas_call(
        functools.partial(attention_kernel, layer, bool(aliases)),
        out_shape=(jax.ShapeDtypeStruct(hidden.shape, hidden.dtype), jax.ShapeDtypeStruct(k_cache.shape, k_cache.dtype), jax.ShapeDtypeStruct(v_cache.shape, v_cache.dtype)),
        in_specs=specs,
        out_specs=(vmem, hbm, hbm),
        input_output_aliases=aliases,
        scratch_shapes=[
            pltpu.VMEM((4 * chunks, model, COLS), jnp.bfloat16),
            pltpu.VMEM(cache_shape, jnp.bfloat16),
            pltpu.VMEM(cache_shape, jnp.bfloat16),
            pltpu.VMEM((3, seqs, model), jnp.float32),
            pltpu.VMEM((seqs * heads, head_dim), jnp.float32),
            pltpu.VMEM((seqs * heads, head_dim), jnp.float32),
            pltpu.VMEM((seqs * heads, head_dim), jnp.float32),
            pltpu.VMEM((seqs * heads, head_dim), jnp.float32),
            pltpu.VMEM((seqs, model), jnp.bfloat16),
            pltpu.SemaphoreType.DMA((4 * chunks,)),
            pltpu.SemaphoreType.DMA((2, CACHE_BLOCKS)),
            pltpu.SemaphoreType.DMA((2, CACHE_BLOCKS)),
        ],
        compiler_params=pltpu.CompilerParams(vmem_limit_bytes=67043328),
        name='attention_layer',
    )(*operands)


def moe_kernel(groups, layer, x_ref, routes_ref, gain_ref, wr_ref, wg, wu, wd, out_ref, ring, rows, xg, act, ys, smat, meta, meta_in, part, dbuf, tbuf, f1, f2, ring_sem, ag_send, ag_recv, meta_send, meta_recv, rs_send, rs_recv):
    seqs, model = x_ref.shape
    local_experts = wg.shape[0]
    experts = wr_ref.shape[1]
    ffn = wg.shape[2]
    slots = xg.shape[1] // groups
    chips = groups // 2
    me = lax.axis_index('ep')
    chip, core = me // 2, me % 2
    step = 1 - 2 * core
    partner = chip * 2 + 1 - core

    def device(offset, core_idx):
        return ((chip + offset + chips) % chips) * 2 + core_idx

    long_dev, short_dev, far_dev = device(step, core), device(-step, core), device(2 * step, core)
    gate_units = 2 * model // UNIT
    down_units = model // UNIT
    total_gate = gate_units * local_experts

    def gate_copy(expert, j):
        weights = wg if j < gate_units // 2 else wu
        slot = (expert * gate_units + j) % RING
        return pltpu.make_async_copy(weights.at[expert, pl.ds((j % (gate_units // 2)) * UNIT, UNIT), :], ring.at[slot], ring_sem.at[slot])

    def down_slot(unit):
        return (total_gate + unit) % RING

    def down_copy(unit):
        half, expert = unit // local_experts, unit % local_experts
        slot = down_slot(unit)
        return pltpu.make_async_copy(wd.at[expert, :, pl.ds(pl.multiple_of(half * UNIT, UNIT), UNIT)], ring.at[slot], ring_sem.at[slot])

    ahead = RING // gate_units
    for expert in range(ahead):
        for j in range(gate_units):
            gate_copy(expert, j).start()

    barrier = pltpu.get_barrier_semaphore()
    for j in range(1, groups):
        pl.semaphore_signal(barrier, inc=1, device_id={'ep': (me + j) % groups}, device_id_type=MESH)

    values = x_ref[...].astype(jnp.float32)
    inv_rms = lax.rsqrt(jnp.mean(values * values, axis=-1, keepdims=True) + RMS_EPS)
    normed = (values * inv_rms * gain_ref[layer:layer + 1, :]).astype(jnp.bfloat16)
    rows[me] = normed
    pl.semaphore_wait(barrier, groups - 1)

    part_rows = seqs // AG_PARTS

    def rows_copy(role, source, peer, q):
        ref = rows.at[source, pl.ds(q * part_rows, part_rows), :]
        return pltpu.make_async_remote_copy(src_ref=ref, dst_ref=ref, send_sem=ag_send.at[role, q], recv_sem=ag_recv.at[role, q], device_id={'ep': peer}, device_id_type=MESH)

    plan = [(me, partner), (me, long_dev), (me, short_dev), (short_dev, long_dev), (short_dev, partner), (long_dev, partner), (far_dev, partner)]
    copies = [[rows_copy(role, source, peer, q) for q in range(AG_PARTS)] for role, (source, peer) in enumerate(plan)]
    for q in range(AG_PARTS):
        for role in (1, 2, 0):
            copies[role][q].start()

    logits = jnp.dot(normed, wr_ref[...], preferred_element_type=jnp.float32)
    shifted = jnp.exp(logits - jnp.max(logits, axis=-1, keepdims=True))
    prob = shifted / jnp.sum(shifted, axis=-1, keepdims=True)
    expert_iota = lax.broadcasted_iota(jnp.int32, (seqs, experts), 1)
    routes = routes_ref[layer]
    chosen = expert_iota == routes[:, 0:1]
    for j in range(1, routes.shape[1]):
        chosen = chosen | (expert_iota == routes[:, j:j + 1])
    row_iota = lax.broadcasted_iota(jnp.int32, (seqs, seqs), 0)
    col_iota = lax.broadcasted_iota(jnp.int32, (seqs, seqs), 1)
    lower = jnp.where(col_iota < row_iota, 1.0, 0.0).astype(jnp.bfloat16)
    ranks = jnp.dot(lower, jnp.where(chosen, 1.0, 0.0).astype(jnp.bfloat16), preferred_element_type=jnp.float32)
    ranks = jnp.where(chosen, ranks, -1.0)
    gates = jnp.where(chosen, prob, 0.0)
    both = jnp.concatenate([jnp.concatenate([ranks, gates], axis=1), jnp.zeros((2 * experts - seqs, 2 * experts), jnp.float32)], axis=0)
    both_t = both.T
    meta[:, :2 * experts] = both_t[:experts]
    meta[:, 2 * experts:] = both_t[experts:]

    def meta_copy(j):
        peer = (me + j) % groups
        return pltpu.make_async_remote_copy(src_ref=meta.at[pl.ds(pl.multiple_of(peer * local_experts, local_experts), local_experts), :], dst_ref=meta_in.at[me], send_sem=meta_send.at[j], recv_sem=meta_recv.at[j], device_id={'ep': peer}, device_id_type=MESH)

    meta_copies = [meta_copy(j) for j in range(1, groups)]
    meta_in[me] = meta[pl.ds(pl.multiple_of(me * local_experts, local_experts), local_experts), :]
    for copy in meta_copies:
        copy.start()

    def gather(source):
        info = meta_in[source]
        rank = info[:, :2 * experts].reshape(local_experts, 1, 2 * experts)
        gate = info[:, 2 * experts:].reshape(local_experts, 1, 2 * experts)
        place = lax.broadcasted_iota(jnp.int32, (local_experts, slots, 2 * experts), 1).astype(jnp.float32)
        hit = jnp.broadcast_to(rank, place.shape) == place
        total = local_experts * slots
        onehot = jnp.where(hit, 1.0, 0.0).reshape(total, 2 * experts)[:, :seqs].astype(jnp.bfloat16)
        taken = jnp.dot(onehot, rows[source], preferred_element_type=jnp.float32).astype(jnp.bfloat16)
        at = pl.ds(pl.multiple_of(source * slots, slots), slots)
        for e in range(local_experts):
            xg[e, at, :] = taken[e * slots:(e + 1) * slots]
        weight = jnp.where(hit, jnp.broadcast_to(gate, place.shape), 0.0).reshape(total, 2 * experts).T[:seqs]
        first = weight.astype(jnp.bfloat16)
        rest = weight - first.astype(jnp.float32)
        second = rest.astype(jnp.bfloat16)
        third = (rest - second.astype(jnp.float32)).astype(jnp.bfloat16)
        smat[source, pl.ds(0, seqs), :] = first
        smat[source, pl.ds(seqs, seqs), :] = second
        smat[source, pl.ds(2 * seqs, seqs), :] = third

    gather(me)
    for q in range(AG_PARTS):
        copies[1][q].wait_recv()
        copies[3][q].start()
        copies[4][q].start()
        copies[2][q].wait_recv()
        copies[5][q].start()
    for copy in meta_copies:
        copy.wait_recv()
    for q in range(AG_PARTS):
        copies[0][q].wait_recv()
    gather(partner)
    gather(short_dev)
    gather(long_dev)
    for role in (4, 5):
        for q in range(AG_PARTS):
            copies[role][q].wait_recv()
    gather(device(step, 1 - core))
    gather(device(-step, 1 - core))
    for q in range(AG_PARTS):
        copies[3][q].wait_recv()
        copies[6][q].start()
    gather(far_dev)
    for q in range(AG_PARTS):
        copies[6][q].wait_recv()
    gather(device(2 * step, 1 - core))

    def expert_body(e, carry):
        def product(first):
            total = None
            for j in range(gate_units // 2):
                slot = (e * gate_units + first + j) % RING
                gate_copy(e, first + j).wait()
                term = jnp.dot(xg[e, :, pl.ds(j * UNIT, UNIT)], ring[slot], preferred_element_type=jnp.float32)
                total = term if total is None else total + term
            return total

        gate_act = product(0)
        up_act = product(gate_units // 2)
        act[e] = (jax.nn.silu(gate_act) * up_act).astype(jnp.bfloat16)

        @pl.when(e + ahead < local_experts)
        def _():
            for j in range(gate_units):
                gate_copy(e + ahead, j).start()

        first_unit = (e + ahead - local_experts) * gate_units

        @pl.when((first_unit >= 0) & (first_unit < down_units * local_experts))
        def _():
            for j in range(gate_units):
                down_copy(first_unit + j).start()

        return carry

    lax.fori_loop(0, local_experts, expert_body, 0)

    width = model // RS_CHUNKS
    per_unit = UNIT // width

    def rs_copy(role, k, source, target, peer):
        return pltpu.make_async_remote_copy(src_ref=source, dst_ref=target, send_sem=rs_send.at[role, k], recv_sem=rs_recv.at[role, k], device_id={'ep': peer}, device_id_type=MESH)

    far_chip, long_chip, short_chip = far_dev // 2, long_dev // 2, short_dev // 2

    def pair_copy(k):
        return rs_copy(0, k, part.at[k, 1 - core], dbuf.at[k], partner)

    def far_copy(k):
        return rs_copy(1, k, part.at[k, core, far_chip], tbuf.at[k], long_dev)

    def short_copy(k):
        return rs_copy(2, k, part.at[k, core, short_chip], f1.at[k], short_dev)

    def long_copy(k):
        return rs_copy(3, k, part.at[k, core, long_chip], f2.at[k], long_dev)

    def compute_chunk(k):
        half = k // per_unit
        column = (k % per_unit) * width

        def down_body(i, carry):
            for u in range(4):
                e = i * 4 + u
                unit = half * local_experts + e
                slot = down_slot(unit)
                if k % per_unit == 0:
                    down_copy(unit).wait()
                out = jnp.dot(act[e], ring[slot, :, pl.ds(column, width)], preferred_element_type=jnp.float32).astype(jnp.bfloat16)
                at = pl.ds(pl.multiple_of(e * slots, slots), slots)
                for b in range(groups):
                    ys[b, at, :] = out[b * slots:(b + 1) * slots]
            return carry

        lax.fori_loop(0, local_experts // 4, down_body, 0)
        for b in range(groups):
            sums = jnp.dot(smat[b], ys[b], preferred_element_type=jnp.float32)
            part[k, b % 2, b // 2] = sums[:seqs] + sums[seqs:2 * seqs] + sums[2 * seqs:]

    def pair_sum(k):
        pair_copy(k).wait_recv()
        part[k, core] = part[k, core] + dbuf[k]
        far_copy(k).start()
        short_copy(k).start()

    def forward(k):
        far_copy(k).wait_recv()
        part[k, core, long_chip] = part[k, core, long_chip] + tbuf[k]
        long_copy(k).start()

    def finish(k):
        short_copy(k).wait_recv()
        long_copy(k).wait_recv()
        moe_out = part[k, core, chip] + f1[k] + f2[k]
        at = pl.ds(k * width, width)
        out_ref[:, at] = (x_ref[:, at].astype(jnp.float32) + moe_out).astype(jnp.bfloat16)

    for k in range(RS_CHUNKS):
        compute_chunk(k)
        pair_copy(k).start()
        if k >= 1:
            pair_sum(k - 1)
        if k >= 2:
            forward(k - 2)
    pair_sum(RS_CHUNKS - 1)
    for k in range(RS_CHUNKS - 2, RS_CHUNKS):
        forward(k)
    for k in range(RS_CHUNKS):
        finish(k)
    for group in copies:
        for copy in group:
            copy.wait_send()
    for copy in meta_copies:
        copy.wait_send()
    for k in range(RS_CHUNKS):
        for make in (pair_copy, far_copy, short_copy, long_copy):
            make(k).wait_send()


def moe_local(hidden, routes, mlp_gain, w_router, w_gate, w_up, w_down, groups, layer):
    seqs, model = hidden.shape
    experts = w_router.shape[1]
    local_experts, _, ffn = w_gate.shape
    slots = CAP_FACTOR * seqs * routes.shape[2] // experts
    chips = groups // 2
    width = model // RS_CHUNKS
    vmem = pl.BlockSpec(memory_space=pltpu.VMEM)
    hbm = pl.BlockSpec(memory_space=pl.ANY)
    return pl.pallas_call(
        functools.partial(moe_kernel, groups, layer),
        out_shape=jax.ShapeDtypeStruct((seqs, model), jnp.bfloat16),
        in_specs=[vmem, vmem, vmem, vmem, hbm, hbm, hbm],
        out_specs=vmem,
        scratch_shapes=[
            pltpu.VMEM((RING, UNIT, ffn), jnp.bfloat16),
            pltpu.VMEM((groups, seqs, model), jnp.bfloat16),
            pltpu.VMEM((local_experts, groups * slots, model), jnp.bfloat16),
            pltpu.VMEM((local_experts, groups * slots, ffn), jnp.bfloat16),
            pltpu.VMEM((groups, local_experts * slots, width), jnp.bfloat16),
            pltpu.VMEM((groups, 3 * seqs, local_experts * slots), jnp.bfloat16),
            pltpu.VMEM((experts, 4 * experts), jnp.float32),
            pltpu.VMEM((groups, local_experts, 4 * experts), jnp.float32),
            pltpu.VMEM((RS_CHUNKS, 2, chips, seqs, width), jnp.float32),
            pltpu.VMEM((RS_CHUNKS, chips, seqs, width), jnp.float32),
            pltpu.VMEM((RS_CHUNKS, seqs, width), jnp.float32),
            pltpu.VMEM((RS_CHUNKS, seqs, width), jnp.float32),
            pltpu.VMEM((RS_CHUNKS, seqs, width), jnp.float32),
            pltpu.SemaphoreType.DMA((RING,)),
            pltpu.SemaphoreType.DMA((7, AG_PARTS)),
            pltpu.SemaphoreType.DMA((7, AG_PARTS)),
            pltpu.SemaphoreType.DMA((groups,)),
            pltpu.SemaphoreType.DMA((groups,)),
            pltpu.SemaphoreType.DMA((4, RS_CHUNKS)),
            pltpu.SemaphoreType.DMA((4, RS_CHUNKS)),
        ],
        compiler_params=pltpu.CompilerParams(collective_id=layer, has_side_effects=True, vmem_limit_bytes=67043328),
        name='moe_layer',
    )(hidden, routes, mlp_gain, w_router, w_gate, w_up, w_down)


def solution(mesh):
    groups = mesh.shape['ep']
    batch_axes = ('dp', 'ep')

    def device_step(hidden, positions, expert_ids, k_cache, v_cache, w_query, w_key, w_value, w_out, attn_gain, q_gain, k_gain, mlp_gain, w_router, w_gate, w_up, w_down):
        cosines, sines = rope_tables(positions, k_cache.shape[4])
        k_new, v_new = None, None
        for layer in range(expert_ids.shape[0]):
            hidden, k_new, v_new = attention_local(layer, hidden, positions, cosines, sines, attn_gain, q_gain, k_gain, w_query, w_key, w_value, w_out, k_cache, v_cache, k_new, v_new)
            hidden = moe_local(hidden, expert_ids, mlp_gain, w_router, w_gate, w_up, w_down, groups, layer)
        return hidden, k_new, v_new

    row_spec = P(batch_axes, None)
    cache_spec = P(None, batch_axes, None, None, None)
    full_spec = P()
    expert_spec = P('ep', None, None)
    in_specs = (row_spec, P(batch_axes), P(None, batch_axes, None), cache_spec, cache_spec, full_spec, full_spec, full_spec, full_spec, full_spec, full_spec, full_spec, full_spec, full_spec, expert_spec, expert_spec, expert_spec)
    return jax.shard_map(device_step, mesh=mesh, in_specs=in_specs, out_specs=(row_spec, cache_spec, cache_spec), check_vma=False)
```

```python
import functools

import jax
import jax.numpy as jnp
import numpy as np
from jax import lax
from jax.experimental import pallas as pl
from jax.experimental.pallas import tpu as pltpu
from jax.sharding import PartitionSpec as P

RMS_EPS = 1e-5
ROPE_BASE = 10000.0
CAP_FACTOR = 2
MESH = pl.DeviceIdType.MESH
AG_PARTS = 2
RS_CHUNKS = 8
UNIT = 1024
RING = 20
LANES = 128
FORWARD_LAG = 5
COLS = 512
CACHE_BLOCKS = 4
ATTEND_UNROLL = 8


def rms_norm(values, gain_vec):
    values = values.astype(jnp.float32)
    inv_rms = lax.rsqrt(jnp.mean(values * values, axis=-1, keepdims=True) + RMS_EPS)
    return values * inv_rms * gain_vec.astype(jnp.float32)


def rope_table(length, head_dim):
    half_dim = head_dim // 2
    frequencies = np.float32(ROPE_BASE) ** (-np.arange(half_dim, dtype=np.float32) / np.float32(half_dim))
    angles = np.arange(length, dtype=np.float32)[:, None] * frequencies[None, :]
    cosines, sines = np.cos(angles), np.sin(angles)
    return np.concatenate([np.concatenate([cosines, cosines], axis=1), np.concatenate([-sines, sines], axis=1)], axis=0).astype(np.float32)


def attention_kernel(layer, aliased, pos_ref, x_ref, table_ref, attn_gain, q_gain, k_gain, wq, wk, wv, wo, k_in, v_in, *rest):
    rest = rest[2:] if aliased else rest
    x_out, k_out, v_out, wbuf, kbuf, vbuf, proj, q_rows, k_rows, v_rows, mixed_rows, mixed, cos_ref, sin_ref, w_sem, in_sem, out_sem = rest
    seqs, model = x_ref.shape
    cache_len, heads, head_dim = kbuf.shape[1:]
    cols = wbuf.shape[2]
    chunks = model // cols
    block = seqs // CACHE_BLOCKS

    def weight_copy(index):
        weights = (wq, wk, wv, wo)[index // chunks]
        return pltpu.make_async_copy(weights.at[layer, :, pl.ds((index % chunks) * cols, cols)], wbuf.at[index], w_sem.at[index])

    def cache_in(kind, i):
        source, target = ((k_in, kbuf), (v_in, vbuf))[kind]
        part = pl.ds(i * block, block)
        return pltpu.make_async_copy(source.at[layer, part], target.at[part], in_sem.at[kind, i])

    def cache_out(kind, i):
        source, target = ((kbuf, k_out), (vbuf, v_out))[kind]
        part = pl.ds(i * block, block)
        return pltpu.make_async_copy(source.at[part], target.at[layer, part], out_sem.at[kind, i])

    for index in range(3 * chunks):
        weight_copy(index).start()
    for i in range(CACHE_BLOCKS):
        for kind in range(2):
            cache_in(kind, i).start()
    for index in range(3 * chunks, 4 * chunks):
        weight_copy(index).start()

    for b in range(seqs):
        position = pos_ref[b]
        cos_ref[b:b + 1, :] = table_ref[pl.ds(position, 1), :]
        sin_ref[b:b + 1, :] = table_ref[pl.ds(position + cache_len, 1), :]
    normed = rms_norm(x_ref[...], attn_gain[layer:layer + 1, :]).astype(jnp.bfloat16)

    def project(kind):
        for c in range(chunks):
            if c % 2 == 0:
                weight_copy(kind * chunks + c).wait()
                weight_copy(kind * chunks + c + 1).wait()
            proj[kind, :, c * cols:(c + 1) * cols] = jnp.dot(normed, wbuf[kind * chunks + c], preferred_element_type=jnp.float32)

    def rotate(kind, gain, target):
        values = proj[kind]
        inv_rms = lax.rsqrt(jnp.mean(values * values, axis=-1, keepdims=True) + RMS_EPS)
        cosines, sines = cos_ref[...], sin_ref[...]
        for h in range(heads):
            at = slice(h * head_dim, (h + 1) * head_dim)
            head = proj[kind, :, at] * inv_rms * gain[layer:layer + 1, at]
            turned = head * cosines + pltpu.roll(head, head_dim // 2, 1) * sines
            target[pl.ds(h, seqs, stride=heads), :] = turned.astype(jnp.bfloat16).astype(jnp.float32)

    project(0)
    rotate(0, q_gain, q_rows)
    project(1)
    rotate(1, k_gain, k_rows)
    project(2)
    for h in range(heads):
        v_rows[pl.ds(h, seqs, stride=heads), :] = proj[2, :, h * head_dim:(h + 1) * head_dim]

    scale = head_dim ** -0.5
    row_iota = lax.broadcasted_iota(jnp.int32, (cache_len, heads, 1), 0)

    def attend(b):
        position = pos_ref[b]
        at = pl.ds(pl.multiple_of(b * heads, heads), heads)
        kbuf[b, position] = k_rows[at, :].astype(jnp.bfloat16)
        vbuf[b, position] = v_rows[at, :].astype(jnp.bfloat16)
        scores = jnp.sum(kbuf[b].astype(jnp.float32) * q_rows[at, :][None], axis=-1, keepdims=True) * scale
        scores = jnp.where(row_iota <= position, scores, -1e30)
        weights = jnp.exp(scores - jnp.max(scores, axis=0, keepdims=True))
        prob = (weights / jnp.sum(weights, axis=0, keepdims=True)).astype(jnp.bfloat16).astype(jnp.float32)
        mixed_rows[at, :] = jnp.sum(prob * vbuf[b].astype(jnp.float32), axis=0)

    for i in range(CACHE_BLOCKS):
        for kind in range(2):
            cache_in(kind, i).wait()

        def body(step, carry):
            for u in range(ATTEND_UNROLL):
                attend(i * block + step * ATTEND_UNROLL + u)
            return carry

        lax.fori_loop(0, block // ATTEND_UNROLL, body, 0)
        for kind in range(2):
            cache_out(kind, i).start()

    for h in range(heads):
        mixed[:, h * head_dim:(h + 1) * head_dim] = mixed_rows[pl.ds(h, seqs, stride=heads), :].astype(jnp.bfloat16)
    for c in range(chunks):
        weight_copy(3 * chunks + c).wait()
    for c in range(chunks):
        at = slice(c * cols, (c + 1) * cols)
        added = jnp.dot(mixed[...], wbuf[3 * chunks + c], preferred_element_type=jnp.float32)
        x_out[:, at] = (x_ref[:, at].astype(jnp.float32) + added).astype(jnp.bfloat16)
    for i in range(CACHE_BLOCKS):
        for kind in range(2):
            cache_out(kind, i).wait()


def attention_local(layer, hidden, positions, table, attn_gain, q_gain, k_gain, w_query, w_key, w_value, w_out, k_cache, v_cache, k_new, v_new):
    seqs, model = hidden.shape
    cache_shape = k_cache.shape[1:]
    heads, head_dim = cache_shape[2:]
    vmem = pl.BlockSpec(memory_space=pltpu.VMEM)
    smem = pl.BlockSpec(memory_space=pltpu.SMEM)
    hbm = pl.BlockSpec(memory_space=pl.ANY)
    operands = [positions, hidden, table, attn_gain, q_gain, k_gain, w_query, w_key, w_value, w_out, k_cache, v_cache]
    specs = [smem] + [vmem] * 5 + [hbm] * 6
    aliases = {}
    if k_new is not None:
        aliases = {len(operands): 1, len(operands) + 1: 2}
        operands += [k_new, v_new]
        specs += [hbm, hbm]
    chunks = model // COLS
    return pl.pallas_call(
        functools.partial(attention_kernel, layer, bool(aliases)),
        out_shape=(jax.ShapeDtypeStruct(hidden.shape, hidden.dtype), jax.ShapeDtypeStruct(k_cache.shape, k_cache.dtype), jax.ShapeDtypeStruct(v_cache.shape, v_cache.dtype)),
        in_specs=specs,
        out_specs=(vmem, hbm, hbm),
        input_output_aliases=aliases,
        scratch_shapes=[
            pltpu.VMEM((4 * chunks, model, COLS), jnp.bfloat16),
            pltpu.VMEM(cache_shape, jnp.bfloat16),
            pltpu.VMEM(cache_shape, jnp.bfloat16),
            pltpu.VMEM((3, seqs, model), jnp.float32),
            pltpu.VMEM((seqs * heads, head_dim), jnp.float32),
            pltpu.VMEM((seqs * heads, head_dim), jnp.float32),
            pltpu.VMEM((seqs * heads, head_dim), jnp.float32),
            pltpu.VMEM((seqs * heads, head_dim), jnp.float32),
            pltpu.VMEM((seqs, model), jnp.bfloat16),
            pltpu.VMEM((seqs, head_dim), jnp.float32),
            pltpu.VMEM((seqs, head_dim), jnp.float32),
            pltpu.SemaphoreType.DMA((4 * chunks,)),
            pltpu.SemaphoreType.DMA((2, CACHE_BLOCKS)),
            pltpu.SemaphoreType.DMA((2, CACHE_BLOCKS)),
        ],
        compiler_params=pltpu.CompilerParams(vmem_limit_bytes=67043328),
        name='attention_layer',
    )(*operands)


def moe_kernel(groups, layer, x_ref, routes_ref, gain_ref, wr_ref, wg, wu, wd, out_ref, ring, rows, xg, act, ys, smat, meta, meta_in, part, dbuf, tbuf, f1, f2, ring_sem, down_sem, ag_send, ag_recv, meta_send, meta_recv, rs_send, rs_recv):
    seqs, model = x_ref.shape
    local_experts = wg.shape[0]
    experts = wr_ref.shape[0]
    ffn = wg.shape[2]
    slots = xg.shape[1] // groups
    chips = groups // 2
    me = lax.axis_index('ep')
    chip, core = me // 2, me % 2
    step = 1 - 2 * core
    partner = chip * 2 + 1 - core

    def device(offset, core_idx):
        return ((chip + offset + chips) % chips) * 2 + core_idx

    long_dev, short_dev, far_dev = device(step, core), device(-step, core), device(2 * step, core)
    gate_units = 2 * model // UNIT
    down_units = model // UNIT
    total_gate = gate_units * local_experts
    width = model // RS_CHUNKS
    per_unit = UNIT // width

    def gate_copy(expert, j):
        weights = wg if j < gate_units // 2 else wu
        slot = (expert * gate_units + j) % RING
        return pltpu.make_async_copy(weights.at[expert, pl.ds((j % (gate_units // 2)) * UNIT, UNIT), :], ring.at[slot], ring_sem.at[slot])

    def down_slot(unit):
        return (total_gate + unit) % RING

    def down_copy(unit, c):
        half, expert = unit // local_experts, unit % local_experts
        slot = down_slot(unit)
        return pltpu.make_async_copy(wd.at[expert, :, pl.ds(half * UNIT + c * width, width)], ring.at[slot, :, pl.ds(c * width, width)], down_sem.at[unit, c])

    ahead = RING // gate_units
    for expert in range(ahead):
        for j in range(gate_units):
            gate_copy(expert, j).start()

    barrier = pltpu.get_barrier_semaphore()
    for j in range(1, groups):
        pl.semaphore_signal(barrier, inc=1, device_id={'ep': (me + j) % groups}, device_id_type=MESH)

    values = x_ref[...].astype(jnp.float32)
    inv_rms = lax.rsqrt(jnp.mean(values * values, axis=-1, keepdims=True) + RMS_EPS)
    normed = (values * inv_rms * gain_ref[layer:layer + 1, :]).astype(jnp.bfloat16)
    rows[me] = normed
    pl.semaphore_wait(barrier, groups - 1)

    part_rows = seqs // AG_PARTS

    def rows_copy(role, source, peer, q):
        ref = rows.at[source, pl.ds(q * part_rows, part_rows), :]
        return pltpu.make_async_remote_copy(src_ref=ref, dst_ref=ref, send_sem=ag_send.at[role, q], recv_sem=ag_recv.at[role, q], device_id={'ep': peer}, device_id_type=MESH)

    plan = [(me, partner), (me, long_dev), (me, short_dev), (short_dev, long_dev), (short_dev, partner), (long_dev, partner), (far_dev, partner)]
    copies = [[rows_copy(role, source, peer, q) for q in range(AG_PARTS)] for role, (source, peer) in enumerate(plan)]
    for q in range(AG_PARTS):
        for role in (1, 2, 0):
            copies[role][q].start()

    logits = lax.dot_general(wr_ref[...], normed, (((1,), (1,)), ((), ())), preferred_element_type=jnp.float32)
    shifted = jnp.exp(logits - jnp.max(logits, axis=0, keepdims=True))
    prob = shifted / jnp.sum(shifted, axis=0, keepdims=True)
    expert_iota = lax.broadcasted_iota(jnp.int32, (experts, seqs), 0)
    routes = routes_ref[layer]
    chosen = expert_iota == routes[0:1, :]
    for j in range(1, routes.shape[0]):
        chosen = chosen | (expert_iota == routes[j:j + 1, :])
    row_iota = lax.broadcasted_iota(jnp.int32, (seqs, seqs), 0)
    col_iota = lax.broadcasted_iota(jnp.int32, (seqs, seqs), 1)
    upper = jnp.where(row_iota < col_iota, 1.0, 0.0).astype(jnp.bfloat16)
    ranks = jnp.dot(jnp.where(chosen, 1.0, 0.0).astype(jnp.bfloat16), upper, preferred_element_type=jnp.float32)
    fill = jnp.zeros((experts, LANES - seqs), jnp.float32)
    meta[:, :LANES] = jnp.concatenate([jnp.where(chosen, ranks, -1.0), fill - 1.0], axis=1)
    meta[:, LANES:] = jnp.concatenate([jnp.where(chosen, prob, 0.0), fill], axis=1)

    def meta_copy(j):
        peer = (me + j) % groups
        return pltpu.make_async_remote_copy(src_ref=meta.at[pl.ds(pl.multiple_of(peer * local_experts, local_experts), local_experts), :], dst_ref=meta_in.at[me], send_sem=meta_send.at[j], recv_sem=meta_recv.at[j], device_id={'ep': peer}, device_id_type=MESH)

    meta_copies = [meta_copy(j) for j in range(1, groups)]
    meta_in[me] = meta[pl.ds(pl.multiple_of(me * local_experts, local_experts), local_experts), :]
    for copy in meta_copies:
        copy.start()

    def gather(source):
        info = meta_in[source]
        rank = info[:, :LANES].reshape(local_experts, 1, LANES)
        gate = info[:, LANES:].reshape(local_experts, 1, LANES)
        place = lax.broadcasted_iota(jnp.int32, (local_experts, slots, LANES), 1).astype(jnp.float32)
        hit = jnp.broadcast_to(rank, place.shape) == place
        total = local_experts * slots
        onehot = jnp.where(hit, 1.0, 0.0).reshape(total, LANES)[:, :seqs].astype(jnp.bfloat16)
        taken = jnp.dot(onehot, rows[source], preferred_element_type=jnp.float32).astype(jnp.bfloat16)
        at = pl.ds(pl.multiple_of(source * slots, slots), slots)
        for e in range(local_experts):
            xg[e, at, :] = taken[e * slots:(e + 1) * slots]
        weight = jnp.where(hit, jnp.broadcast_to(gate, place.shape), 0.0).reshape(total, LANES).T[:seqs]
        first = weight.astype(jnp.bfloat16)
        rest = weight - first.astype(jnp.float32)
        second = rest.astype(jnp.bfloat16)
        third = (rest - second.astype(jnp.float32)).astype(jnp.bfloat16)
        smat[source, pl.ds(0, seqs), :] = first
        smat[source, pl.ds(seqs, seqs), :] = second
        smat[source, pl.ds(2 * seqs, seqs), :] = third

    gather(me)
    for q in range(AG_PARTS):
        copies[1][q].wait_recv()
        copies[3][q].start()
        copies[4][q].start()
        copies[2][q].wait_recv()
        copies[5][q].start()
    for copy in meta_copies:
        copy.wait_recv()
    for q in range(AG_PARTS):
        copies[0][q].wait_recv()
    gather(partner)
    gather(short_dev)
    gather(long_dev)
    for role in (4, 5):
        for q in range(AG_PARTS):
            copies[role][q].wait_recv()
    gather(device(step, 1 - core))
    gather(device(-step, 1 - core))
    for q in range(AG_PARTS):
        copies[3][q].wait_recv()
        copies[6][q].start()
    gather(far_dev)
    for q in range(AG_PARTS):
        copies[6][q].wait_recv()
    gather(device(2 * step, 1 - core))

    def expert_body(e, carry):
        for j in range(gate_units):
            gate_copy(e, j).wait()

        def product(first):
            total = None
            for j in range(gate_units // 2):
                slot = (e * gate_units + first + j) % RING
                term = jnp.dot(xg[e, :, pl.ds(j * UNIT, UNIT)], ring[slot], preferred_element_type=jnp.float32)
                total = term if total is None else total + term
            return total

        gate_act = product(0)
        up_act = product(gate_units // 2)
        act[e] = (jax.nn.silu(gate_act) * up_act).astype(jnp.bfloat16)

        @pl.when(e + ahead < local_experts)
        def _():
            for j in range(gate_units):
                gate_copy(e + ahead, j).start()

        for half in range(down_units):
            freed = (half + 1) * local_experts // gate_units + local_experts - ahead - 1

            @pl.when(e == freed)
            def _():
                for c in range(per_unit):
                    for expert in range(local_experts):
                        down_copy(half * local_experts + expert, c).start()

        return carry

    lax.fori_loop(0, local_experts, expert_body, 0)

    def rs_copy(role, k, source, target, peer):
        return pltpu.make_async_remote_copy(src_ref=source, dst_ref=target, send_sem=rs_send.at[role, k], recv_sem=rs_recv.at[role, k], device_id={'ep': peer}, device_id_type=MESH)

    far_chip, long_chip, short_chip = far_dev // 2, long_dev // 2, short_dev // 2

    def pair_copy(k):
        return rs_copy(0, k, part.at[k, 1 - core], dbuf.at[k], partner)

    def far_copy(k):
        return rs_copy(1, k, part.at[k, core, far_chip], tbuf.at[k], long_dev)

    def short_copy(k):
        return rs_copy(2, k, part.at[k, core, short_chip], f1.at[k], short_dev)

    def long_copy(k):
        return rs_copy(3, k, part.at[k, core, long_chip], f2.at[k], long_dev)

    def compute_chunk(k):
        half = k // per_unit
        column = (k % per_unit) * width

        units = [half * local_experts + e for e in range(local_experts)]
        for unit in units:
            down_copy(unit, k % per_unit).wait()
        for e, unit in enumerate(units):
            out = jnp.dot(act[e], ring[down_slot(unit), :, column:column + width], preferred_element_type=jnp.float32).astype(jnp.bfloat16)
            for b in range(groups):
                ys[b, e * slots:(e + 1) * slots, :] = out[b * slots:(b + 1) * slots]
        for b in range(groups):
            sums = jnp.dot(smat[b], ys[b], preferred_element_type=jnp.float32)
            part[k, b % 2, b // 2] = sums[:seqs] + sums[seqs:2 * seqs] + sums[2 * seqs:]

    def pair_sum(k):
        pair_copy(k).wait_recv()
        part[k, core] = part[k, core] + dbuf[k]
        far_copy(k).start()
        short_copy(k).start()

    def forward(k):
        far_copy(k).wait_recv()
        part[k, core, long_chip] = part[k, core, long_chip] + tbuf[k]
        long_copy(k).start()

    def finish(k):
        short_copy(k).wait_recv()
        long_copy(k).wait_recv()
        moe_out = part[k, core, chip] + f1[k] + f2[k]
        at = pl.ds(k * width, width)
        out_ref[:, at] = (x_ref[:, at].astype(jnp.float32) + moe_out).astype(jnp.bfloat16)

    for k in range(RS_CHUNKS):
        compute_chunk(k)
        pair_copy(k).start()
        if k >= 1:
            pair_sum(k - 1)
        if k >= FORWARD_LAG:
            forward(k - FORWARD_LAG)
    pair_sum(RS_CHUNKS - 1)
    for k in range(RS_CHUNKS - FORWARD_LAG, RS_CHUNKS):
        forward(k)
    for k in range(RS_CHUNKS):
        finish(k)
    for group in copies:
        for copy in group:
            copy.wait_send()
    for copy in meta_copies:
        copy.wait_send()
    for k in range(RS_CHUNKS):
        for make in (pair_copy, far_copy, short_copy, long_copy):
            make(k).wait_send()


def moe_local(hidden, routes, mlp_gain, w_router, w_gate, w_up, w_down, groups, layer):
    seqs, model = hidden.shape
    experts = w_router.shape[0]
    local_experts, _, ffn = w_gate.shape
    slots = CAP_FACTOR * seqs * routes.shape[1] // experts
    chips = groups // 2
    width = model // RS_CHUNKS
    vmem = pl.BlockSpec(memory_space=pltpu.VMEM)
    hbm = pl.BlockSpec(memory_space=pl.ANY)
    return pl.pallas_call(
        functools.partial(moe_kernel, groups, layer),
        out_shape=jax.ShapeDtypeStruct((seqs, model), jnp.bfloat16),
        in_specs=[vmem, vmem, vmem, vmem, hbm, hbm, hbm],
        out_specs=vmem,
        scratch_shapes=[
            pltpu.VMEM((RING, UNIT, ffn), jnp.bfloat16),
            pltpu.VMEM((groups, seqs, model), jnp.bfloat16),
            pltpu.VMEM((local_experts, groups * slots, model), jnp.bfloat16),
            pltpu.VMEM((local_experts, groups * slots, ffn), jnp.bfloat16),
            pltpu.VMEM((groups, local_experts * slots, width), jnp.bfloat16),
            pltpu.VMEM((groups, 3 * seqs, local_experts * slots), jnp.bfloat16),
            pltpu.VMEM((experts, 2 * LANES), jnp.float32),
            pltpu.VMEM((groups, local_experts, 2 * LANES), jnp.float32),
            pltpu.VMEM((RS_CHUNKS, 2, chips, seqs, width), jnp.float32),
            pltpu.VMEM((RS_CHUNKS, chips, seqs, width), jnp.float32),
            pltpu.VMEM((RS_CHUNKS, seqs, width), jnp.float32),
            pltpu.VMEM((RS_CHUNKS, seqs, width), jnp.float32),
            pltpu.VMEM((RS_CHUNKS, seqs, width), jnp.float32),
            pltpu.SemaphoreType.DMA((RING,)),
            pltpu.SemaphoreType.DMA((model // UNIT * local_experts, UNIT // width)),
            pltpu.SemaphoreType.DMA((7, AG_PARTS)),
            pltpu.SemaphoreType.DMA((7, AG_PARTS)),
            pltpu.SemaphoreType.DMA((groups,)),
            pltpu.SemaphoreType.DMA((groups,)),
            pltpu.SemaphoreType.DMA((4, RS_CHUNKS)),
            pltpu.SemaphoreType.DMA((4, RS_CHUNKS)),
        ],
        compiler_params=pltpu.CompilerParams(collective_id=layer, has_side_effects=True, vmem_limit_bytes=67043328),
        name='moe_layer',
    )(hidden, routes, mlp_gain, w_router, w_gate, w_up, w_down)


def solution(mesh):
    groups = mesh.shape['ep']
    batch_axes = ('dp', 'ep')

    def device_step(hidden, positions, expert_ids, k_cache, v_cache, w_query, w_key, w_value, w_out, attn_gain, q_gain, k_gain, mlp_gain, w_router, w_gate, w_up, w_down):
        table = jnp.asarray(rope_table(k_cache.shape[2], k_cache.shape[4]))
        routes = jnp.swapaxes(expert_ids, 1, 2)
        router = w_router.T
        k_new, v_new = None, None
        for layer in range(expert_ids.shape[0]):
            hidden, k_new, v_new = attention_local(layer, hidden, positions, table, attn_gain, q_gain, k_gain, w_query, w_key, w_value, w_out, k_cache, v_cache, k_new, v_new)
            hidden = moe_local(hidden, routes, mlp_gain, router, w_gate, w_up, w_down, groups, layer)
        return hidden, k_new, v_new

    row_spec = P(batch_axes, None)
    cache_spec = P(None, batch_axes, None, None, None)
    full_spec = P()
    expert_spec = P('ep', None, None)
    in_specs = (row_spec, P(batch_axes), P(None, batch_axes, None), cache_spec, cache_spec, full_spec, full_spec, full_spec, full_spec, full_spec, full_spec, full_spec, full_spec, full_spec, expert_spec, expert_spec, expert_spec)
    return jax.shard_map(device_step, mesh=mesh, in_specs=in_specs, out_specs=(row_spec, cache_spec, cache_spec), check_vma=False)
```

```python
import functools

import jax
import jax.numpy as jnp
import numpy as np
from jax import lax
from jax.experimental import pallas as pl
from jax.experimental.pallas import tpu as pltpu
from jax.sharding import PartitionSpec as P

RMS_EPS = 1e-5
ROPE_BASE = 10000.0
CAP_FACTOR = 2
MESH = pl.DeviceIdType.MESH
AG_PARTS = 2
RS_CHUNKS = 8
UNIT = 1024
RING = 20
LANES = 128
FORWARD_LAG = 5
COLS = 512
CACHE_BLOCKS = 4
SCORE_UNROLL = 8
MIX_UNROLL = 8
WO_AFTER = 1


def rms_norm(values, gain_vec):
    values = values.astype(jnp.float32)
    inv_rms = lax.rsqrt(jnp.mean(values * values, axis=-1, keepdims=True) + RMS_EPS)
    return values * inv_rms * gain_vec.astype(jnp.float32)


def rope_table(length, head_dim):
    half_dim = head_dim // 2
    frequencies = np.float32(ROPE_BASE) ** (-np.arange(half_dim, dtype=np.float32) / np.float32(half_dim))
    angles = np.arange(length, dtype=np.float32)[:, None] * frequencies[None, :]
    cosines, sines = np.cos(angles), np.sin(angles)
    return np.concatenate([np.concatenate([cosines, cosines], axis=1), np.concatenate([-sines, sines], axis=1)], axis=0).astype(np.float32)


def attention_kernel(layer, aliased, pos_ref, x_ref, table_ref, attn_gain, q_gain, k_gain, wq, wk, wv, wo, k_in, v_in, *rest):
    rest = rest[2:] if aliased else rest
    x_hbm, k_out, v_out, x_out, x_sem, wbuf, kbuf, vbuf, proj, q_rows, k_rows, v_rows, mixed_rows, mixed, probs, cos_ref, sin_ref, w_sem, in_sem, out_sem = rest
    seqs, model = x_ref.shape
    cache_len, heads, head_dim = kbuf.shape[1:]
    cols = wbuf.shape[2]
    chunks = model // cols
    block = seqs // CACHE_BLOCKS

    def weight_copy(index):
        if not isinstance(index, int):
            at = pl.ds(pl.multiple_of((index - 2 * chunks) * cols, cols), cols)
            return pltpu.make_async_copy(wv.at[layer, :, at], wbuf.at[index], w_sem.at[index])
        weights = (wq, wk, wv, wo)[index // chunks]
        return pltpu.make_async_copy(weights.at[layer, :, pl.ds((index % chunks) * cols, cols)], wbuf.at[index], w_sem.at[index])

    def cache_in(kind, i):
        source, target = ((k_in, kbuf), (v_in, vbuf))[kind]
        part = pl.ds(i * block, block)
        return pltpu.make_async_copy(source.at[layer, part], target.at[part], in_sem.at[kind, i])

    def cache_out(kind, i):
        source, target = ((kbuf, k_out), (vbuf, v_out))[kind]
        part = pl.ds(i * block, block)
        return pltpu.make_async_copy(source.at[part], target.at[layer, part], out_sem.at[kind, i])

    for index in range(2 * chunks):
        weight_copy(index).start()
    later = [[cache_in(0, i) for i in range(CACHE_BLOCKS)], [weight_copy(index) for index in range(2 * chunks, 3 * chunks)], [cache_in(1, i) for i in range(CACHE_BLOCKS)]]

    def issue_next():
        if later:
            for copy in later.pop(0):
                copy.start()


    for b in range(seqs):
        position = pos_ref[b]
        cos_ref[b:b + 1, :] = table_ref[pl.ds(position, 1), :]
        sin_ref[b:b + 1, :] = table_ref[pl.ds(position + cache_len, 1), :]
    normed = rms_norm(x_ref[...], attn_gain[layer:layer + 1, :]).astype(jnp.bfloat16)

    def project(kind):
        for c in range(chunks):
            if c % 2 == 0:
                weight_copy(kind * chunks + c).wait()
                weight_copy(kind * chunks + c + 1).wait()
                issue_next()
            proj[kind, :, c * cols:(c + 1) * cols] = jnp.dot(normed, wbuf[kind * chunks + c], preferred_element_type=jnp.float32)

    def rotate(kind, gain, target):
        values = proj[kind]
        inv_rms = lax.rsqrt(jnp.mean(values * values, axis=-1, keepdims=True) + RMS_EPS)
        cosines, sines = cos_ref[...], sin_ref[...]
        for h in range(heads):
            at = slice(h * head_dim, (h + 1) * head_dim)
            head = proj[kind, :, at] * inv_rms * gain[layer:layer + 1, at]
            turned = head * cosines + pltpu.roll(head, head_dim // 2, 1) * sines
            target[pl.ds(h, seqs, stride=heads), :] = turned.astype(jnp.bfloat16).astype(jnp.float32)

    project(0)
    rotate(0, q_gain, q_rows)
    project(1)
    rotate(1, k_gain, k_rows)

    scale = head_dim ** -0.5
    row_iota = lax.broadcasted_iota(jnp.int32, (cache_len, heads, 1), 0)

    def rows_of(b):
        return pl.ds(pl.multiple_of(b * heads, heads), heads)

    def score(b):
        position = pos_ref[b]
        kbuf[b, position] = k_rows[rows_of(b), :].astype(jnp.bfloat16)
        scores = jnp.sum(kbuf[b].astype(jnp.float32) * q_rows[rows_of(b), :][None], axis=-1, keepdims=True) * scale
        scores = jnp.where(row_iota <= position, scores, -1e30)
        weights = jnp.exp(scores - jnp.max(scores, axis=0, keepdims=True))
        prob = weights / jnp.sum(weights, axis=0, keepdims=True)
        probs[b] = jnp.broadcast_to(prob, probs.shape[1:]).astype(jnp.bfloat16)

    def mix(b):
        vbuf[b, pos_ref[b]] = v_rows[rows_of(b), :].astype(jnp.bfloat16)
        mixed_rows[rows_of(b), :] = jnp.sum(probs[b].astype(jnp.float32) * vbuf[b].astype(jnp.float32), axis=0)

    def value_chunk(c):
        weight_copy(2 * chunks + c).wait()
        at = pl.ds(pl.multiple_of(c * cols, cols), cols)
        proj[2, :, at] = jnp.dot(normed, wbuf[2 * chunks + c], preferred_element_type=jnp.float32)

    trips = CACHE_BLOCKS * (block // SCORE_UNROLL)

    def sweep(kind, step, unroll):
        for i in range(CACHE_BLOCKS):
            cache_in(kind, i).wait()
            if kind == 0 and i == WO_AFTER:
                for index in range(3 * chunks, 4 * chunks):
                    weight_copy(index).start()

            def body(outer, carry):
                first = trips - chunks
                trip = i * (block // unroll)
                if kind == 0 and trip >= first:
                    value_chunk(trip - first + outer)
                for u in range(unroll):
                    step(i * block + outer * unroll + u)
                return carry

            lax.fori_loop(0, block // unroll, body, 0)
            if kind == 1:
                cache_out(0, i).start()
                cache_out(1, i).start()

    sweep(0, score, SCORE_UNROLL)
    for h in range(heads):
        v_rows[pl.ds(h, seqs, stride=heads), :] = proj[2, :, h * head_dim:(h + 1) * head_dim]
    sweep(1, mix, MIX_UNROLL)
    for h in range(heads):
        mixed[:, h * head_dim:(h + 1) * head_dim] = mixed_rows[pl.ds(h, seqs, stride=heads), :].astype(jnp.bfloat16)
    for c in range(chunks):
        weight_copy(3 * chunks + c).wait()
    for c in range(chunks):
        at = slice(c * cols, (c + 1) * cols)
        added = jnp.dot(mixed[...], wbuf[3 * chunks + c], preferred_element_type=jnp.float32)
        x_out[:, at] = (x_ref[:, at].astype(jnp.float32) + added).astype(jnp.bfloat16)
    result = pltpu.make_async_copy(x_out, x_hbm, x_sem)
    result.start()
    for i in range(CACHE_BLOCKS):
        for kind in range(2):
            cache_out(kind, i).wait()
    result.wait()


def attention_local(layer, hidden, positions, table, attn_gain, q_gain, k_gain, w_query, w_key, w_value, w_out, k_cache, v_cache, k_new, v_new):
    seqs, model = hidden.shape
    cache_shape = k_cache.shape[1:]
    heads, head_dim = cache_shape[2:]
    vmem = pl.BlockSpec(memory_space=pltpu.VMEM)
    smem = pl.BlockSpec(memory_space=pltpu.SMEM)
    hbm = pl.BlockSpec(memory_space=pl.ANY)
    operands = [positions, hidden, table, attn_gain, q_gain, k_gain, w_query, w_key, w_value, w_out, k_cache, v_cache]
    specs = [smem] + [vmem] * 5 + [hbm] * 6
    aliases = {}
    if k_new is not None:
        aliases = {len(operands): 1, len(operands) + 1: 2}
        operands += [k_new, v_new]
        specs += [hbm, hbm]
    chunks = model // COLS
    return pl.pallas_call(
        functools.partial(attention_kernel, layer, bool(aliases)),
        out_shape=(jax.ShapeDtypeStruct(hidden.shape, hidden.dtype), jax.ShapeDtypeStruct(k_cache.shape, k_cache.dtype), jax.ShapeDtypeStruct(v_cache.shape, v_cache.dtype)),
        in_specs=specs,
        out_specs=(hbm, hbm, hbm),
        input_output_aliases=aliases,
        scratch_shapes=[
            pltpu.VMEM(hidden.shape, hidden.dtype),
            pltpu.SemaphoreType.DMA,
            pltpu.VMEM((4 * chunks, model, COLS), jnp.bfloat16),
            pltpu.VMEM(cache_shape, jnp.bfloat16),
            pltpu.VMEM(cache_shape, jnp.bfloat16),
            pltpu.VMEM((3, seqs, model), jnp.float32),
            pltpu.VMEM((seqs * heads, head_dim), jnp.float32),
            pltpu.VMEM((seqs * heads, head_dim), jnp.float32),
            pltpu.VMEM((seqs * heads, head_dim), jnp.float32),
            pltpu.VMEM((seqs * heads, head_dim), jnp.float32),
            pltpu.VMEM((seqs, model), jnp.bfloat16),
            pltpu.VMEM(cache_shape, jnp.bfloat16),
            pltpu.VMEM((seqs, head_dim), jnp.float32),
            pltpu.VMEM((seqs, head_dim), jnp.float32),
            pltpu.SemaphoreType.DMA((4 * chunks,)),
            pltpu.SemaphoreType.DMA((2, CACHE_BLOCKS)),
            pltpu.SemaphoreType.DMA((2, CACHE_BLOCKS)),
        ],
        compiler_params=pltpu.CompilerParams(vmem_limit_bytes=67043328),
        name='attention_layer',
    )(*operands)


def moe_kernel(groups, layer, x_ref, routes_ref, gain_ref, wr_ref, wg, wu, wd, out_hbm, out_ref, out_sem, ring, rows, xg, act, ys, smat, meta, meta_in, part, dbuf, tbuf, f1, f2, ring_sem, down_sem, ag_send, ag_recv, meta_send, meta_recv, rs_send, rs_recv):
    seqs, model = x_ref.shape
    local_experts = wg.shape[0]
    experts = wr_ref.shape[0]
    ffn = wg.shape[2]
    slots = xg.shape[1] // groups
    chips = groups // 2
    me = lax.axis_index('ep')
    chip, core = me // 2, me % 2
    step = 1 - 2 * core
    partner = chip * 2 + 1 - core

    def device(offset, core_idx):
        return ((chip + offset + chips) % chips) * 2 + core_idx

    long_dev, short_dev, far_dev = device(step, core), device(-step, core), device(2 * step, core)
    gate_units = 2 * model // UNIT
    down_units = model // UNIT
    total_gate = gate_units * local_experts
    width = model // RS_CHUNKS
    per_unit = UNIT // width

    def gate_copy(expert, j):
        weights = wg if j < gate_units // 2 else wu
        slot = (expert * gate_units + j) % RING
        return pltpu.make_async_copy(weights.at[expert, pl.ds((j % (gate_units // 2)) * UNIT, UNIT), :], ring.at[slot], ring_sem.at[slot])

    def down_slot(unit):
        return (total_gate + unit) % RING

    def down_copy(unit, c):
        half, expert = unit // local_experts, unit % local_experts
        slot = down_slot(unit)
        return pltpu.make_async_copy(wd.at[expert, :, pl.ds(half * UNIT + c * width, width)], ring.at[slot, :, pl.ds(c * width, width)], down_sem.at[unit, c])

    ahead = RING // gate_units
    for expert in range(ahead):
        for j in range(gate_units):
            gate_copy(expert, j).start()

    barrier = pltpu.get_barrier_semaphore()
    for j in range(1, groups):
        pl.semaphore_signal(barrier, inc=1, device_id={'ep': (me + j) % groups}, device_id_type=MESH)

    values = x_ref[...].astype(jnp.float32)
    inv_rms = lax.rsqrt(jnp.mean(values * values, axis=-1, keepdims=True) + RMS_EPS)
    normed = (values * inv_rms * gain_ref[layer:layer + 1, :]).astype(jnp.bfloat16)
    rows[me] = normed
    pl.semaphore_wait(barrier, groups - 1)

    part_rows = seqs // AG_PARTS

    def rows_copy(role, source, peer, q):
        ref = rows.at[source, pl.ds(q * part_rows, part_rows), :]
        return pltpu.make_async_remote_copy(src_ref=ref, dst_ref=ref, send_sem=ag_send.at[role, q], recv_sem=ag_recv.at[role, q], device_id={'ep': peer}, device_id_type=MESH)

    plan = [(me, partner), (me, long_dev), (me, short_dev), (short_dev, long_dev), (short_dev, partner), (long_dev, partner), (far_dev, partner)]
    copies = [[rows_copy(role, source, peer, q) for q in range(AG_PARTS)] for role, (source, peer) in enumerate(plan)]
    for q in range(AG_PARTS):
        for role in (1, 2, 0):
            copies[role][q].start()

    logits = lax.dot_general(wr_ref[...], normed, (((1,), (1,)), ((), ())), preferred_element_type=jnp.float32)
    shifted = jnp.exp(logits - jnp.max(logits, axis=0, keepdims=True))
    prob = shifted / jnp.sum(shifted, axis=0, keepdims=True)
    expert_iota = lax.broadcasted_iota(jnp.int32, (experts, seqs), 0)
    routes = routes_ref[layer]
    chosen = expert_iota == routes[0:1, :]
    for j in range(1, routes.shape[0]):
        chosen = chosen | (expert_iota == routes[j:j + 1, :])
    row_iota = lax.broadcasted_iota(jnp.int32, (seqs, seqs), 0)
    col_iota = lax.broadcasted_iota(jnp.int32, (seqs, seqs), 1)
    upper = jnp.where(row_iota < col_iota, 1.0, 0.0).astype(jnp.bfloat16)
    ranks = jnp.dot(jnp.where(chosen, 1.0, 0.0).astype(jnp.bfloat16), upper, preferred_element_type=jnp.float32)
    fill = jnp.zeros((experts, LANES - seqs), jnp.float32)
    meta[:, :LANES] = jnp.concatenate([jnp.where(chosen, ranks, -1.0), fill - 1.0], axis=1)
    meta[:, LANES:] = jnp.concatenate([jnp.where(chosen, prob, 0.0), fill], axis=1)

    def meta_copy(j):
        peer = (me + j) % groups
        return pltpu.make_async_remote_copy(src_ref=meta.at[pl.ds(pl.multiple_of(peer * local_experts, local_experts), local_experts), :], dst_ref=meta_in.at[me], send_sem=meta_send.at[j], recv_sem=meta_recv.at[j], device_id={'ep': peer}, device_id_type=MESH)

    meta_copies = [meta_copy(j) for j in range(1, groups)]
    meta_in[me] = meta[pl.ds(pl.multiple_of(me * local_experts, local_experts), local_experts), :]
    for copy in meta_copies:
        copy.start()

    def gather(source):
        info = meta_in[source]
        rank = info[:, :LANES].reshape(local_experts, 1, LANES)
        gate = info[:, LANES:].reshape(local_experts, 1, LANES)
        place = lax.broadcasted_iota(jnp.int32, (local_experts, slots, LANES), 1).astype(jnp.float32)
        hit = jnp.broadcast_to(rank, place.shape) == place
        total = local_experts * slots
        onehot = jnp.where(hit, 1.0, 0.0).reshape(total, LANES)[:, :seqs].astype(jnp.bfloat16)
        taken = jnp.dot(onehot, rows[source], preferred_element_type=jnp.float32).astype(jnp.bfloat16)
        at = pl.ds(pl.multiple_of(source * slots, slots), slots)
        for e in range(local_experts):
            xg[e, at, :] = taken[e * slots:(e + 1) * slots]
        weight = jnp.where(hit, jnp.broadcast_to(gate, place.shape), 0.0).reshape(total, LANES).T[:seqs]
        first = weight.astype(jnp.bfloat16)
        rest = weight - first.astype(jnp.float32)
        second = rest.astype(jnp.bfloat16)
        third = (rest - second.astype(jnp.float32)).astype(jnp.bfloat16)
        smat[source, pl.ds(0, seqs), :] = first
        smat[source, pl.ds(seqs, seqs), :] = second
        smat[source, pl.ds(2 * seqs, seqs), :] = third

    gather(me)
    for q in range(AG_PARTS):
        copies[1][q].wait_recv()
        copies[3][q].start()
        copies[4][q].start()
        copies[2][q].wait_recv()
        copies[5][q].start()
    for copy in meta_copies:
        copy.wait_recv()
    for q in range(AG_PARTS):
        copies[0][q].wait_recv()
    gather(partner)
    gather(short_dev)
    gather(long_dev)
    for role in (4, 5):
        for q in range(AG_PARTS):
            copies[role][q].wait_recv()
    gather(device(step, 1 - core))
    gather(device(-step, 1 - core))
    for q in range(AG_PARTS):
        copies[3][q].wait_recv()
        copies[6][q].start()
    gather(far_dev)
    for q in range(AG_PARTS):
        copies[6][q].wait_recv()
    gather(device(2 * step, 1 - core))

    def expert_body(e, carry):
        for j in range(gate_units):
            gate_copy(e, j).wait()

        def product(first):
            total = None
            for j in range(gate_units // 2):
                slot = (e * gate_units + first + j) % RING
                term = jnp.dot(xg[e, :, pl.ds(j * UNIT, UNIT)], ring[slot], preferred_element_type=jnp.float32)
                total = term if total is None else total + term
            return total

        gate_act = product(0)
        up_act = product(gate_units // 2)
        act[e] = (jax.nn.silu(gate_act) * up_act).astype(jnp.bfloat16)

        @pl.when(e + ahead < local_experts)
        def _():
            for j in range(gate_units):
                gate_copy(e + ahead, j).start()

        for half in range(down_units):
            freed = (half + 1) * local_experts // gate_units + local_experts - ahead - 1

            @pl.when(e == freed)
            def _():
                for c in range(per_unit):
                    for expert in range(local_experts):
                        down_copy(half * local_experts + expert, c).start()

        return carry

    lax.fori_loop(0, local_experts, expert_body, 0)

    def rs_copy(role, k, source, target, peer):
        return pltpu.make_async_remote_copy(src_ref=source, dst_ref=target, send_sem=rs_send.at[role, k], recv_sem=rs_recv.at[role, k], device_id={'ep': peer}, device_id_type=MESH)

    far_chip, long_chip, short_chip = far_dev // 2, long_dev // 2, short_dev // 2

    def pair_copy(k):
        return rs_copy(0, k, part.at[k, 1 - core], dbuf.at[k], partner)

    def far_copy(k):
        return rs_copy(1, k, part.at[k, core, far_chip], tbuf.at[k], long_dev)

    def short_copy(k):
        return rs_copy(2, k, part.at[k, core, short_chip], f1.at[k], short_dev)

    def long_copy(k):
        return rs_copy(3, k, part.at[k, core, long_chip], f2.at[k], long_dev)

    def compute_chunk(k):
        half = k // per_unit
        column = (k % per_unit) * width

        units = [half * local_experts + e for e in range(local_experts)]
        for unit in units:
            down_copy(unit, k % per_unit).wait()
        for e, unit in enumerate(units):
            out = jnp.dot(act[e], ring[down_slot(unit), :, column:column + width], preferred_element_type=jnp.float32).astype(jnp.bfloat16)
            for b in range(groups):
                ys[b, e * slots:(e + 1) * slots, :] = out[b * slots:(b + 1) * slots]
        for b in range(groups):
            sums = jnp.dot(smat[b], ys[b], preferred_element_type=jnp.float32)
            part[k, b % 2, b // 2] = sums[:seqs] + sums[seqs:2 * seqs] + sums[2 * seqs:]

    def pair_sum(k):
        pair_copy(k).wait_recv()
        part[k, core] = part[k, core] + dbuf[k]
        far_copy(k).start()
        short_copy(k).start()

    def forward(k):
        far_copy(k).wait_recv()
        part[k, core, long_chip] = part[k, core, long_chip] + tbuf[k]
        long_copy(k).start()

    def finish(k):
        short_copy(k).wait_recv()
        long_copy(k).wait_recv()
        moe_out = part[k, core, chip] + f1[k] + f2[k]
        at = pl.ds(k * width, width)
        out_ref[:, at] = (x_ref[:, at].astype(jnp.float32) + moe_out).astype(jnp.bfloat16)

    for k in range(RS_CHUNKS):
        compute_chunk(k)
        pair_copy(k).start()
        if k >= 1:
            pair_sum(k - 1)
        if k >= FORWARD_LAG:
            forward(k - FORWARD_LAG)
    pair_sum(RS_CHUNKS - 1)
    for group in copies:
        for copy in group:
            copy.wait_send()
    for copy in meta_copies:
        copy.wait_send()
    for k in range(RS_CHUNKS - FORWARD_LAG):
        for make in (pair_copy, far_copy, short_copy):
            make(k).wait_send()
    for k in range(RS_CHUNKS - FORWARD_LAG, RS_CHUNKS):
        forward(k)
    for k in range(RS_CHUNKS):
        finish(k)
    result = pltpu.make_async_copy(out_ref, out_hbm, out_sem)
    result.start()
    for k in range(RS_CHUNKS):
        if k >= RS_CHUNKS - FORWARD_LAG:
            for make in (pair_copy, far_copy, short_copy):
                make(k).wait_send()
        long_copy(k).wait_send()
    result.wait()


def moe_local(hidden, routes, mlp_gain, w_router, w_gate, w_up, w_down, groups, layer):
    seqs, model = hidden.shape
    experts = w_router.shape[0]
    local_experts, _, ffn = w_gate.shape
    slots = CAP_FACTOR * seqs * routes.shape[1] // experts
    chips = groups // 2
    width = model // RS_CHUNKS
    vmem = pl.BlockSpec(memory_space=pltpu.VMEM)
    hbm = pl.BlockSpec(memory_space=pl.ANY)
    return pl.pallas_call(
        functools.partial(moe_kernel, groups, layer),
        out_shape=jax.ShapeDtypeStruct((seqs, model), jnp.bfloat16),
        in_specs=[vmem, vmem, vmem, vmem, hbm, hbm, hbm],
        out_specs=hbm,
        scratch_shapes=[
            pltpu.VMEM((seqs, model), jnp.bfloat16),
            pltpu.SemaphoreType.DMA,
            pltpu.VMEM((RING, UNIT, ffn), jnp.bfloat16),
            pltpu.VMEM((groups, seqs, model), jnp.bfloat16),
            pltpu.VMEM((local_experts, groups * slots, model), jnp.bfloat16),
            pltpu.VMEM((local_experts, groups * slots, ffn), jnp.bfloat16),
            pltpu.VMEM((groups, local_experts * slots, width), jnp.bfloat16),
            pltpu.VMEM((groups, 3 * seqs, local_experts * slots), jnp.bfloat16),
            pltpu.VMEM((experts, 2 * LANES), jnp.float32),
            pltpu.VMEM((groups, local_experts, 2 * LANES), jnp.float32),
            pltpu.VMEM((RS_CHUNKS, 2, chips, seqs, width), jnp.float32),
            pltpu.VMEM((RS_CHUNKS, chips, seqs, width), jnp.float32),
            pltpu.VMEM((RS_CHUNKS, seqs, width), jnp.float32),
            pltpu.VMEM((RS_CHUNKS, seqs, width), jnp.float32),
            pltpu.VMEM((RS_CHUNKS, seqs, width), jnp.float32),
            pltpu.SemaphoreType.DMA((RING,)),
            pltpu.SemaphoreType.DMA((model // UNIT * local_experts, UNIT // width)),
            pltpu.SemaphoreType.DMA((7, AG_PARTS)),
            pltpu.SemaphoreType.DMA((7, AG_PARTS)),
            pltpu.SemaphoreType.DMA((groups,)),
            pltpu.SemaphoreType.DMA((groups,)),
            pltpu.SemaphoreType.DMA((4, RS_CHUNKS)),
            pltpu.SemaphoreType.DMA((4, RS_CHUNKS)),
        ],
        compiler_params=pltpu.CompilerParams(collective_id=layer, has_side_effects=True, vmem_limit_bytes=67043328),
        name='moe_layer',
    )(hidden, routes, mlp_gain, w_router, w_gate, w_up, w_down)


def solution(mesh):
    groups = mesh.shape['ep']
    batch_axes = ('dp', 'ep')

    def device_step(hidden, positions, expert_ids, k_cache, v_cache, w_query, w_key, w_value, w_out, attn_gain, q_gain, k_gain, mlp_gain, w_router, w_gate, w_up, w_down):
        table = jnp.asarray(rope_table(k_cache.shape[2], k_cache.shape[4]))
        routes = jnp.swapaxes(expert_ids, 1, 2)
        router = w_router.T
        k_new, v_new = None, None
        for layer in range(expert_ids.shape[0]):
            hidden, k_new, v_new = attention_local(layer, hidden, positions, table, attn_gain, q_gain, k_gain, w_query, w_key, w_value, w_out, k_cache, v_cache, k_new, v_new)
            hidden = moe_local(hidden, routes, mlp_gain, router, w_gate, w_up, w_down, groups, layer)
        return hidden, k_new, v_new

    row_spec = P(batch_axes, None)
    cache_spec = P(None, batch_axes, None, None, None)
    full_spec = P()
    expert_spec = P('ep', None, None)
    in_specs = (row_spec, P(batch_axes), P(None, batch_axes, None), cache_spec, cache_spec, full_spec, full_spec, full_spec, full_spec, full_spec, full_spec, full_spec, full_spec, full_spec, expert_spec, expert_spec, expert_spec)
    return jax.shard_map(device_step, mesh=mesh, in_specs=in_specs, out_specs=(row_spec, cache_spec, cache_spec), check_vma=False)
```

```python
import functools

import jax
import jax.numpy as jnp
import numpy as np
from jax import lax
from jax.experimental import pallas as pl
from jax.experimental.pallas import tpu as pltpu
from jax.sharding import PartitionSpec as P

RMS_EPS = 1e-5
ROPE_BASE = 10000.0
CAP_FACTOR = 2
MESH = pl.DeviceIdType.MESH
AG_PARTS = 4
RS_CHUNKS = 8
UNIT = 1024
RING = 20
LANES = 128
FORWARD_LAG = 5
COLS = 512
CACHE_BLOCKS = 4
SCORE_UNROLL = 8
MIX_UNROLL = 8
WO_AFTER = 1


def rms_norm(values, gain_vec):
    values = values.astype(jnp.float32)
    inv_rms = lax.rsqrt(jnp.mean(values * values, axis=-1, keepdims=True) + RMS_EPS)
    return values * inv_rms * gain_vec.astype(jnp.float32)


def rope_table(length, head_dim):
    half_dim = head_dim // 2
    frequencies = np.float32(ROPE_BASE) ** (-np.arange(half_dim, dtype=np.float32) / np.float32(half_dim))
    angles = np.arange(length, dtype=np.float32)[:, None] * frequencies[None, :]
    cosines, sines = np.cos(angles), np.sin(angles)
    return np.concatenate([np.concatenate([cosines, cosines], axis=1), np.concatenate([-sines, sines], axis=1)], axis=0).astype(np.float32)


def attention_kernel(layer, aliased, pos_ref, x_ref, table_ref, attn_gain, q_gain, k_gain, wq, wk, wv, wo, k_in, v_in, *rest):
    rest = rest[2:] if aliased else rest
    x_hbm, k_out, v_out, x_out, x_sem, wbuf, kbuf, vbuf, proj, q_rows, k_rows, v_rows, mixed_rows, mixed, probs, cos_ref, sin_ref, w_sem, in_sem, out_sem = rest
    seqs, model = x_ref.shape
    cache_len, heads, head_dim = kbuf.shape[1:]
    cols = wbuf.shape[2]
    chunks = model // cols
    block = seqs // CACHE_BLOCKS

    def weight_copy(index):
        if not isinstance(index, int):
            at = pl.ds(pl.multiple_of((index - 2 * chunks) * cols, cols), cols)
            return pltpu.make_async_copy(wv.at[layer, :, at], wbuf.at[index], w_sem.at[index])
        weights = (wq, wk, wv, wo)[index // chunks]
        return pltpu.make_async_copy(weights.at[layer, :, pl.ds((index % chunks) * cols, cols)], wbuf.at[index], w_sem.at[index])

    def cache_in(kind, i):
        source, target = ((k_in, kbuf), (v_in, vbuf))[kind]
        part = pl.ds(i * block, block)
        return pltpu.make_async_copy(source.at[layer, part], target.at[part], in_sem.at[kind, i])

    def cache_out(kind, i):
        source, target = ((kbuf, k_out), (vbuf, v_out))[kind]
        part = pl.ds(i * block, block)
        return pltpu.make_async_copy(source.at[part], target.at[layer, part], out_sem.at[kind, i])

    for index in range(2 * chunks):
        weight_copy(index).start()
    later = [[cache_in(0, i) for i in range(CACHE_BLOCKS)], [weight_copy(index) for index in range(2 * chunks, 3 * chunks)], [cache_in(1, i) for i in range(CACHE_BLOCKS)]]

    def issue_next():
        if later:
            for copy in later.pop(0):
                copy.start()


    for b in range(seqs):
        position = pos_ref[b]
        cos_ref[b:b + 1, :] = table_ref[pl.ds(position, 1), :]
        sin_ref[b:b + 1, :] = table_ref[pl.ds(position + cache_len, 1), :]
    normed = rms_norm(x_ref[...], attn_gain[layer:layer + 1, :]).astype(jnp.bfloat16)

    def project(kind):
        for c in range(chunks):
            if c % 2 == 0:
                weight_copy(kind * chunks + c).wait()
                weight_copy(kind * chunks + c + 1).wait()
                issue_next()
            proj[kind, :, c * cols:(c + 1) * cols] = jnp.dot(normed, wbuf[kind * chunks + c], preferred_element_type=jnp.float32)

    def rotate(kind, gain, target, factor):
        values = proj[kind]
        inv_rms = lax.rsqrt(jnp.mean(values * values, axis=-1, keepdims=True) + RMS_EPS)
        cosines, sines = cos_ref[...], sin_ref[...]
        for h in range(heads):
            at = slice(h * head_dim, (h + 1) * head_dim)
            head = proj[kind, :, at] * inv_rms * gain[layer:layer + 1, at]
            turned = head * cosines + pltpu.roll(head, head_dim // 2, 1) * sines
            target[pl.ds(h, seqs, stride=heads), :] = turned.astype(jnp.bfloat16).astype(jnp.float32) * factor

    project(0)
    rotate(0, q_gain, q_rows, head_dim ** -0.5)
    project(1)
    rotate(1, k_gain, k_rows, 1.0)

    row_iota = lax.broadcasted_iota(jnp.int32, (cache_len, heads, 1), 0)

    def rows_of(b):
        return pl.ds(pl.multiple_of(b * heads, heads), heads)

    def score(b):
        position = pos_ref[b]
        kbuf[b, position] = k_rows[rows_of(b), :].astype(jnp.bfloat16)
        scores = jnp.sum(kbuf[b].astype(jnp.float32) * q_rows[rows_of(b), :][None], axis=-1, keepdims=True)
        scores = jnp.where(row_iota <= position, scores, -1e30)
        weights = jnp.exp(scores - jnp.max(scores, axis=0, keepdims=True))
        prob = weights * (1.0 / jnp.sum(weights, axis=0, keepdims=True))
        probs[b] = jnp.broadcast_to(prob, probs.shape[1:]).astype(jnp.bfloat16)

    def mix(b):
        vbuf[b, pos_ref[b]] = v_rows[rows_of(b), :].astype(jnp.bfloat16)
        mixed_rows[rows_of(b), :] = jnp.sum(probs[b].astype(jnp.float32) * vbuf[b].astype(jnp.float32), axis=0)

    def value_chunk(c):
        weight_copy(2 * chunks + c).wait()
        at = pl.ds(pl.multiple_of(c * cols, cols), cols)
        proj[2, :, at] = jnp.dot(normed, wbuf[2 * chunks + c], preferred_element_type=jnp.float32)

    trips = CACHE_BLOCKS * (block // SCORE_UNROLL)

    def sweep(kind, step, unroll):
        for i in range(CACHE_BLOCKS):
            cache_in(kind, i).wait()
            if kind == 0 and i == WO_AFTER:
                for index in range(3 * chunks, 4 * chunks):
                    weight_copy(index).start()

            def body(outer, carry):
                first = trips - chunks
                trip = i * (block // unroll)
                if kind == 0 and trip >= first:
                    value_chunk(trip - first + outer)
                for u in range(unroll):
                    step(i * block + outer * unroll + u)
                return carry

            lax.fori_loop(0, block // unroll, body, 0)
            if kind == 1:
                cache_out(0, i).start()
                cache_out(1, i).start()

    sweep(0, score, SCORE_UNROLL)
    for h in range(heads):
        v_rows[pl.ds(h, seqs, stride=heads), :] = proj[2, :, h * head_dim:(h + 1) * head_dim]
    sweep(1, mix, MIX_UNROLL)
    for h in range(heads):
        mixed[:, h * head_dim:(h + 1) * head_dim] = mixed_rows[pl.ds(h, seqs, stride=heads), :].astype(jnp.bfloat16)
    for c in range(chunks):
        if c % 2 == 0:
            weight_copy(3 * chunks + c).wait()
            weight_copy(3 * chunks + c + 1).wait()
        at = slice(c * cols, (c + 1) * cols)
        added = jnp.dot(mixed[...], wbuf[3 * chunks + c], preferred_element_type=jnp.float32)
        x_out[:, at] = (x_ref[:, at].astype(jnp.float32) + added).astype(jnp.bfloat16)
    result = pltpu.make_async_copy(x_out, x_hbm, x_sem)
    result.start()
    for i in range(CACHE_BLOCKS):
        for kind in range(2):
            cache_out(kind, i).wait()
    result.wait()


def attention_local(layer, hidden, positions, table, attn_gain, q_gain, k_gain, w_query, w_key, w_value, w_out, k_cache, v_cache, k_new, v_new):
    seqs, model = hidden.shape
    cache_shape = k_cache.shape[1:]
    heads, head_dim = cache_shape[2:]
    vmem = pl.BlockSpec(memory_space=pltpu.VMEM)
    smem = pl.BlockSpec(memory_space=pltpu.SMEM)
    hbm = pl.BlockSpec(memory_space=pl.ANY)
    operands = [positions, hidden, table, attn_gain, q_gain, k_gain, w_query, w_key, w_value, w_out, k_cache, v_cache]
    specs = [smem] + [vmem] * 5 + [hbm] * 6
    aliases = {}
    if k_new is not None:
        aliases = {len(operands): 1, len(operands) + 1: 2}
        operands += [k_new, v_new]
        specs += [hbm, hbm]
    chunks = model // COLS
    return pl.pallas_call(
        functools.partial(attention_kernel, layer, bool(aliases)),
        out_shape=(jax.ShapeDtypeStruct(hidden.shape, hidden.dtype), jax.ShapeDtypeStruct(k_cache.shape, k_cache.dtype), jax.ShapeDtypeStruct(v_cache.shape, v_cache.dtype)),
        in_specs=specs,
        out_specs=(hbm, hbm, hbm),
        input_output_aliases=aliases,
        scratch_shapes=[
            pltpu.VMEM(hidden.shape, hidden.dtype),
            pltpu.SemaphoreType.DMA,
            pltpu.VMEM((4 * chunks, model, COLS), jnp.bfloat16),
            pltpu.VMEM(cache_shape, jnp.bfloat16),
            pltpu.VMEM(cache_shape, jnp.bfloat16),
            pltpu.VMEM((3, seqs, model), jnp.float32),
            pltpu.VMEM((seqs * heads, head_dim), jnp.float32),
            pltpu.VMEM((seqs * heads, head_dim), jnp.float32),
            pltpu.VMEM((seqs * heads, head_dim), jnp.float32),
            pltpu.VMEM((seqs * heads, head_dim), jnp.float32),
            pltpu.VMEM((seqs, model), jnp.bfloat16),
            pltpu.VMEM(cache_shape, jnp.bfloat16),
            pltpu.VMEM((seqs, head_dim), jnp.float32),
            pltpu.VMEM((seqs, head_dim), jnp.float32),
            pltpu.SemaphoreType.DMA((4 * chunks,)),
            pltpu.SemaphoreType.DMA((2, CACHE_BLOCKS)),
            pltpu.SemaphoreType.DMA((2, CACHE_BLOCKS)),
        ],
        compiler_params=pltpu.CompilerParams(vmem_limit_bytes=67043328),
        name='attention_layer',
    )(*operands)


def moe_kernel(groups, layer, x_ref, routes_ref, gain_ref, wr_ref, wg, wu, wd, out_hbm, out_ref, out_sem, ring, rows, xg, act, ys, smat, meta, meta_in, part, dbuf, tbuf, f1, f2, ring_sem, down_sem, ag_send, ag_recv, meta_send, meta_recv, rs_send, rs_recv):
    seqs, model = x_ref.shape
    local_experts = wg.shape[0]
    experts = wr_ref.shape[0]
    ffn = wg.shape[2]
    slots = xg.shape[1] // groups
    chips = groups // 2
    me = lax.axis_index('ep')
    chip, core = me // 2, me % 2
    step = 1 - 2 * core
    partner = chip * 2 + 1 - core

    def device(offset, core_idx):
        return ((chip + offset + chips) % chips) * 2 + core_idx

    long_dev, short_dev, far_dev = device(step, core), device(-step, core), device(2 * step, core)
    gate_units = 2 * model // UNIT
    down_units = model // UNIT
    total_gate = gate_units * local_experts
    width = model // RS_CHUNKS
    per_unit = UNIT // width

    def gate_copy(expert, j):
        weights = wg if j < gate_units // 2 else wu
        slot = (expert * gate_units + j) % RING
        return pltpu.make_async_copy(weights.at[expert, pl.ds((j % (gate_units // 2)) * UNIT, UNIT), :], ring.at[slot], ring_sem.at[slot])

    def down_slot(unit):
        return (total_gate + unit) % RING

    def down_copy(unit, c):
        half, expert = unit // local_experts, unit % local_experts
        slot = down_slot(unit)
        return pltpu.make_async_copy(wd.at[expert, :, pl.ds(half * UNIT + c * width, width)], ring.at[slot, :, pl.ds(c * width, width)], down_sem.at[unit, c])

    ahead = RING // gate_units
    for expert in range(ahead):
        for j in range(gate_units):
            gate_copy(expert, j).start()

    barrier = pltpu.get_barrier_semaphore()
    for j in range(1, groups):
        pl.semaphore_signal(barrier, inc=1, device_id={'ep': (me + j) % groups}, device_id_type=MESH)

    values = x_ref[...].astype(jnp.float32)
    inv_rms = lax.rsqrt(jnp.mean(values * values, axis=-1, keepdims=True) + RMS_EPS)
    normed = (values * inv_rms * gain_ref[layer:layer + 1, :]).astype(jnp.bfloat16)
    rows[me] = normed
    pl.semaphore_wait(barrier, groups - 1)

    part_rows = seqs // AG_PARTS

    def rows_copy(role, source, peer, q):
        ref = rows.at[source, pl.ds(q * part_rows, part_rows), :]
        return pltpu.make_async_remote_copy(src_ref=ref, dst_ref=ref, send_sem=ag_send.at[role, q], recv_sem=ag_recv.at[role, q], device_id={'ep': peer}, device_id_type=MESH)

    plan = [(me, partner), (me, long_dev), (me, short_dev), (short_dev, long_dev), (short_dev, partner), (long_dev, partner), (far_dev, partner)]
    copies = [[rows_copy(role, source, peer, q) for q in range(AG_PARTS)] for role, (source, peer) in enumerate(plan)]
    for q in range(AG_PARTS):
        for role in (1, 2, 0):
            copies[role][q].start()

    logits = lax.dot_general(wr_ref[...], normed, (((1,), (1,)), ((), ())), preferred_element_type=jnp.float32)
    shifted = jnp.exp(logits - jnp.max(logits, axis=0, keepdims=True))
    prob = shifted / jnp.sum(shifted, axis=0, keepdims=True)
    expert_iota = lax.broadcasted_iota(jnp.int32, (experts, seqs), 0)
    routes = routes_ref[layer]
    chosen = expert_iota == routes[0:1, :]
    for j in range(1, routes.shape[0]):
        chosen = chosen | (expert_iota == routes[j:j + 1, :])
    row_iota = lax.broadcasted_iota(jnp.int32, (seqs, seqs), 0)
    col_iota = lax.broadcasted_iota(jnp.int32, (seqs, seqs), 1)
    upper = jnp.where(row_iota < col_iota, 1.0, 0.0).astype(jnp.bfloat16)
    ranks = jnp.dot(jnp.where(chosen, 1.0, 0.0).astype(jnp.bfloat16), upper, preferred_element_type=jnp.float32)
    fill = jnp.zeros((experts, LANES - seqs), jnp.float32)
    meta[:, :LANES] = jnp.concatenate([jnp.where(chosen, ranks, -1.0), fill - 1.0], axis=1)
    meta[:, LANES:] = jnp.concatenate([jnp.where(chosen, prob, 0.0), fill], axis=1)

    def meta_copy(j):
        peer = (me + j) % groups
        return pltpu.make_async_remote_copy(src_ref=meta.at[pl.ds(pl.multiple_of(peer * local_experts, local_experts), local_experts), :], dst_ref=meta_in.at[me], send_sem=meta_send.at[j], recv_sem=meta_recv.at[j], device_id={'ep': peer}, device_id_type=MESH)

    meta_copies = [meta_copy(j) for j in range(1, groups)]
    meta_in[me] = meta[pl.ds(pl.multiple_of(me * local_experts, local_experts), local_experts), :]
    for copy in meta_copies:
        copy.start()

    def gather(source):
        info = meta_in[source]
        rank = info[:, :LANES].reshape(local_experts, 1, LANES)
        gate = info[:, LANES:].reshape(local_experts, 1, LANES)
        place = lax.broadcasted_iota(jnp.int32, (local_experts, slots, LANES), 1).astype(jnp.float32)
        hit = jnp.broadcast_to(rank, place.shape) == place
        total = local_experts * slots
        onehot = jnp.where(hit, 1.0, 0.0).reshape(total, LANES)[:, :seqs].astype(jnp.bfloat16)
        taken = jnp.dot(onehot, rows[source], preferred_element_type=jnp.float32).astype(jnp.bfloat16)
        at = pl.ds(pl.multiple_of(source * slots, slots), slots)
        for e in range(local_experts):
            xg[e, at, :] = taken[e * slots:(e + 1) * slots]
        weight = jnp.where(hit, jnp.broadcast_to(gate, place.shape), 0.0).reshape(total, LANES).T[:seqs]
        first = weight.astype(jnp.bfloat16)
        rest = weight - first.astype(jnp.float32)
        second = rest.astype(jnp.bfloat16)
        third = (rest - second.astype(jnp.float32)).astype(jnp.bfloat16)
        smat[source, pl.ds(0, seqs), :] = first
        smat[source, pl.ds(seqs, seqs), :] = second
        smat[source, pl.ds(2 * seqs, seqs), :] = third

    gather(me)
    for q in range(AG_PARTS):
        copies[1][q].wait_recv()
        copies[3][q].start()
        copies[4][q].start()
        copies[2][q].wait_recv()
        copies[5][q].start()
    for copy in meta_copies:
        copy.wait_recv()
    for q in range(AG_PARTS):
        copies[0][q].wait_recv()
    gather(partner)
    gather(short_dev)
    gather(long_dev)
    for role in (4, 5):
        for q in range(AG_PARTS):
            copies[role][q].wait_recv()
    gather(device(step, 1 - core))
    gather(device(-step, 1 - core))
    for q in range(AG_PARTS):
        copies[3][q].wait_recv()
        copies[6][q].start()
    gather(far_dev)
    for q in range(AG_PARTS):
        copies[6][q].wait_recv()
    gather(device(2 * step, 1 - core))

    def expert_body(e, carry):
        for j in range(gate_units):
            gate_copy(e, j).wait()

        def product(first):
            total = None
            for j in range(gate_units // 2):
                slot = (e * gate_units + first + j) % RING
                term = jnp.dot(xg[e, :, pl.ds(j * UNIT, UNIT)], ring[slot], preferred_element_type=jnp.float32)
                total = term if total is None else total + term
            return total

        gate_act = product(0)
        up_act = product(gate_units // 2)
        act[e] = (jax.nn.silu(gate_act) * up_act).astype(jnp.bfloat16)

        @pl.when(e + ahead < local_experts)
        def _():
            for j in range(gate_units):
                gate_copy(e + ahead, j).start()

        for half in range(down_units):
            freed = (half + 1) * local_experts // gate_units + local_experts - ahead - 1

            @pl.when(e == freed)
            def _():
                for c in range(per_unit):
                    for expert in range(local_experts):
                        down_copy(half * local_experts + expert, c).start()

        return carry

    lax.fori_loop(0, local_experts, expert_body, 0)

    def rs_copy(role, k, source, target, peer):
        return pltpu.make_async_remote_copy(src_ref=source, dst_ref=target, send_sem=rs_send.at[role, k], recv_sem=rs_recv.at[role, k], device_id={'ep': peer}, device_id_type=MESH)

    far_chip, long_chip, short_chip = far_dev // 2, long_dev // 2, short_dev // 2

    def pair_copy(k):
        return rs_copy(0, k, part.at[k, 1 - core], dbuf.at[k], partner)

    def far_copy(k):
        return rs_copy(1, k, part.at[k, core, far_chip], tbuf.at[k], long_dev)

    def short_copy(k):
        return rs_copy(2, k, part.at[k, core, short_chip], f1.at[k], short_dev)

    def long_copy(k):
        return rs_copy(3, k, part.at[k, core, long_chip], f2.at[k], long_dev)

    def compute_chunk(k):
        half = k // per_unit
        column = (k % per_unit) * width

        units = [half * local_experts + e for e in range(local_experts)]
        for unit in units:
            down_copy(unit, k % per_unit).wait()
        for e, unit in enumerate(units):
            out = jnp.dot(act[e], ring[down_slot(unit), :, column:column + width], preferred_element_type=jnp.float32).astype(jnp.bfloat16)
            for b in range(groups):
                ys[b, e * slots:(e + 1) * slots, :] = out[b * slots:(b + 1) * slots]
        for b in range(groups):
            sums = jnp.dot(smat[b], ys[b], preferred_element_type=jnp.float32)
            part[k, b % 2, b // 2] = sums[:seqs] + sums[seqs:2 * seqs] + sums[2 * seqs:]

    def pair_sum(k):
        pair_copy(k).wait_recv()
        part[k, core] = part[k, core] + dbuf[k]
        far_copy(k).start()
        short_copy(k).start()

    def forward(k):
        far_copy(k).wait_recv()
        part[k, core, long_chip] = part[k, core, long_chip] + tbuf[k]
        long_copy(k).start()

    def finish(k):
        short_copy(k).wait_recv()
        long_copy(k).wait_recv()
        moe_out = part[k, core, chip] + f1[k] + f2[k]
        at = pl.ds(k * width, width)
        out_ref[:, at] = (x_ref[:, at].astype(jnp.float32) + moe_out).astype(jnp.bfloat16)

    for k in range(RS_CHUNKS):
        compute_chunk(k)
        pair_copy(k).start()
        if k >= 1:
            pair_sum(k - 1)
        if k >= FORWARD_LAG:
            forward(k - FORWARD_LAG)
    pair_sum(RS_CHUNKS - 1)
    for group in copies:
        for copy in group:
            copy.wait_send()
    for copy in meta_copies:
        copy.wait_send()
    for k in range(RS_CHUNKS - FORWARD_LAG):
        for make in (pair_copy, far_copy, short_copy):
            make(k).wait_send()
    for k in range(RS_CHUNKS - FORWARD_LAG, RS_CHUNKS):
        forward(k)
    for k in range(RS_CHUNKS):
        finish(k)
    result = pltpu.make_async_copy(out_ref, out_hbm, out_sem)
    result.start()
    for k in range(RS_CHUNKS):
        if k >= RS_CHUNKS - FORWARD_LAG:
            for make in (pair_copy, far_copy, short_copy):
                make(k).wait_send()
        long_copy(k).wait_send()
    result.wait()


def moe_local(hidden, routes, mlp_gain, w_router, w_gate, w_up, w_down, groups, layer):
    seqs, model = hidden.shape
    experts = w_router.shape[0]
    local_experts, _, ffn = w_gate.shape
    slots = CAP_FACTOR * seqs * routes.shape[1] // experts
    chips = groups // 2
    width = model // RS_CHUNKS
    vmem = pl.BlockSpec(memory_space=pltpu.VMEM)
    hbm = pl.BlockSpec(memory_space=pl.ANY)
    return pl.pallas_call(
        functools.partial(moe_kernel, groups, layer),
        out_shape=jax.ShapeDtypeStruct((seqs, model), jnp.bfloat16),
        in_specs=[vmem, vmem, vmem, vmem, hbm, hbm, hbm],
        out_specs=hbm,
        scratch_shapes=[
            pltpu.VMEM((seqs, model), jnp.bfloat16),
            pltpu.SemaphoreType.DMA,
            pltpu.VMEM((RING, UNIT, ffn), jnp.bfloat16),
            pltpu.VMEM((groups, seqs, model), jnp.bfloat16),
            pltpu.VMEM((local_experts, groups * slots, model), jnp.bfloat16),
            pltpu.VMEM((local_experts, groups * slots, ffn), jnp.bfloat16),
            pltpu.VMEM((groups, local_experts * slots, width), jnp.bfloat16),
            pltpu.VMEM((groups, 3 * seqs, local_experts * slots), jnp.bfloat16),
            pltpu.VMEM((experts, 2 * LANES), jnp.float32),
            pltpu.VMEM((groups, local_experts, 2 * LANES), jnp.float32),
            pltpu.VMEM((RS_CHUNKS, 2, chips, seqs, width), jnp.float32),
            pltpu.VMEM((RS_CHUNKS, chips, seqs, width), jnp.float32),
            pltpu.VMEM((RS_CHUNKS, seqs, width), jnp.float32),
            pltpu.VMEM((RS_CHUNKS, seqs, width), jnp.float32),
            pltpu.VMEM((RS_CHUNKS, seqs, width), jnp.float32),
            pltpu.SemaphoreType.DMA((RING,)),
            pltpu.SemaphoreType.DMA((model // UNIT * local_experts, UNIT // width)),
            pltpu.SemaphoreType.DMA((7, AG_PARTS)),
            pltpu.SemaphoreType.DMA((7, AG_PARTS)),
            pltpu.SemaphoreType.DMA((groups,)),
            pltpu.SemaphoreType.DMA((groups,)),
            pltpu.SemaphoreType.DMA((4, RS_CHUNKS)),
            pltpu.SemaphoreType.DMA((4, RS_CHUNKS)),
        ],
        compiler_params=pltpu.CompilerParams(collective_id=layer, has_side_effects=True, vmem_limit_bytes=67043328),
        name='moe_layer',
    )(hidden, routes, mlp_gain, w_router, w_gate, w_up, w_down)


def solution(mesh):
    groups = mesh.shape['ep']
    batch_axes = ('dp', 'ep')

    def device_step(hidden, positions, expert_ids, k_cache, v_cache, w_query, w_key, w_value, w_out, attn_gain, q_gain, k_gain, mlp_gain, w_router, w_gate, w_up, w_down):
        table = jnp.asarray(rope_table(k_cache.shape[2], k_cache.shape[4]))
        routes = jnp.swapaxes(expert_ids, 1, 2)
        router = w_router.T
        k_new, v_new = None, None
        for layer in range(expert_ids.shape[0]):
            hidden, k_new, v_new = attention_local(layer, hidden, positions, table, attn_gain, q_gain, k_gain, w_query, w_key, w_value, w_out, k_cache, v_cache, k_new, v_new)
            hidden = moe_local(hidden, routes, mlp_gain, router, w_gate, w_up, w_down, groups, layer)
        return hidden, k_new, v_new

    row_spec = P(batch_axes, None)
    cache_spec = P(None, batch_axes, None, None, None)
    full_spec = P()
    expert_spec = P('ep', None, None)
    in_specs = (row_spec, P(batch_axes), P(None, batch_axes, None), cache_spec, cache_spec, full_spec, full_spec, full_spec, full_spec, full_spec, full_spec, full_spec, full_spec, full_spec, expert_spec, expert_spec, expert_spec)
    return jax.shard_map(device_step, mesh=mesh, in_specs=in_specs, out_specs=(row_spec, cache_spec, cache_spec), check_vma=False)
```

```python
import functools

import jax
import jax.numpy as jnp
import numpy as np
from jax import lax
from jax.experimental import pallas as pl
from jax.experimental.pallas import tpu as pltpu
from jax.sharding import PartitionSpec as P

RMS_EPS = 1e-5
ROPE_BASE = 10000.0
CAP_FACTOR = 2
MESH = pl.DeviceIdType.MESH
AG_PARTS = 4
RS_CHUNKS = 8
UNIT = 1024
RING = 20
LANES = 128
FORWARD_LAG = 6
COLS = 512
CACHE_BLOCKS = 4
SCORE_UNROLL = 8
MIX_UNROLL = 8
WO_AFTER = 1


def rms_norm(values, gain_vec):
    values = values.astype(jnp.float32)
    inv_rms = lax.rsqrt(jnp.mean(values * values, axis=-1, keepdims=True) + RMS_EPS)
    return values * inv_rms * gain_vec.astype(jnp.float32)


def rope_table(length, head_dim):
    half_dim = head_dim // 2
    frequencies = np.float32(ROPE_BASE) ** (-np.arange(half_dim, dtype=np.float32) / np.float32(half_dim))
    angles = np.arange(length, dtype=np.float32)[:, None] * frequencies[None, :]
    cosines, sines = np.cos(angles), np.sin(angles)
    return np.concatenate([np.concatenate([cosines, cosines], axis=1), np.concatenate([-sines, sines], axis=1)], axis=0).astype(np.float32)


def attention_kernel(layer, aliased, pos_ref, x_ref, table_ref, attn_gain, q_gain, k_gain, wq, wk, wv, wo, k_in, v_in, *rest):
    rest = rest[2:] if aliased else rest
    x_hbm, k_out, v_out, x_out, x_sem, wbuf, kbuf, vbuf, proj, q_rows, k_rows, v_rows, mixed_rows, mixed, probs, cos_ref, sin_ref, w_sem, in_sem, out_sem = rest
    seqs, model = x_ref.shape
    cache_len, heads, head_dim = kbuf.shape[1:]
    cols = wbuf.shape[2]
    chunks = model // cols
    block = seqs // CACHE_BLOCKS

    def weight_copy(index):
        if not isinstance(index, int):
            at = pl.ds(pl.multiple_of((index - 2 * chunks) * cols, cols), cols)
            return pltpu.make_async_copy(wv.at[layer, :, at], wbuf.at[index], w_sem.at[index])
        weights = (wq, wk, wv, wo)[index // chunks]
        return pltpu.make_async_copy(weights.at[layer, :, pl.ds((index % chunks) * cols, cols)], wbuf.at[index], w_sem.at[index])

    def cache_in(kind, i):
        source, target = ((k_in, kbuf), (v_in, vbuf))[kind]
        part = pl.ds(i * block, block)
        return pltpu.make_async_copy(source.at[layer, part], target.at[part], in_sem.at[kind, i])

    def cache_out(kind, i):
        source, target = ((kbuf, k_out), (vbuf, v_out))[kind]
        part = pl.ds(i * block, block)
        return pltpu.make_async_copy(source.at[part], target.at[layer, part], out_sem.at[kind, i])

    for index in range(2 * chunks):
        weight_copy(index).start()
    later = [[cache_in(0, i) for i in range(CACHE_BLOCKS)], [weight_copy(index) for index in range(2 * chunks, 3 * chunks)], [cache_in(1, i) for i in range(CACHE_BLOCKS)]]

    def issue_next():
        if later:
            for copy in later.pop(0):
                copy.start()


    def table_row(b, carry):
        position = pos_ref[b]
        cos_ref[pl.ds(b, 1), :] = table_ref[pl.ds(position, 1), :]
        sin_ref[pl.ds(b, 1), :] = table_ref[pl.ds(position + cache_len, 1), :]
        return carry

    lax.fori_loop(0, seqs, table_row, 0)
    normed = rms_norm(x_ref[...], attn_gain[layer:layer + 1, :]).astype(jnp.bfloat16)

    def project(kind):
        for c in range(chunks):
            if c % 2 == 0:
                weight_copy(kind * chunks + c).wait()
                weight_copy(kind * chunks + c + 1).wait()
                issue_next()
            proj[kind, :, c * cols:(c + 1) * cols] = jnp.dot(normed, wbuf[kind * chunks + c], preferred_element_type=jnp.float32)

    def rotate(kind, gain, target, factor):
        values = proj[kind]
        inv_rms = lax.rsqrt(jnp.mean(values * values, axis=-1, keepdims=True) + RMS_EPS)
        cosines, sines = cos_ref[...], sin_ref[...]
        for h in range(heads):
            at = slice(h * head_dim, (h + 1) * head_dim)
            head = proj[kind, :, at] * inv_rms * gain[layer:layer + 1, at]
            turned = head * cosines + pltpu.roll(head, head_dim // 2, 1) * sines
            target[pl.ds(h, seqs, stride=heads), :] = turned.astype(jnp.bfloat16).astype(jnp.float32) * factor

    project(0)
    rotate(0, q_gain, q_rows, head_dim ** -0.5)
    project(1)
    rotate(1, k_gain, k_rows, 1.0)

    row_iota = lax.broadcasted_iota(jnp.int32, (cache_len, heads, 1), 0)

    def rows_of(b):
        return pl.ds(pl.multiple_of(b * heads, heads), heads)

    def score(b):
        position = pos_ref[b]
        kbuf[b, position] = k_rows[rows_of(b), :].astype(jnp.bfloat16)
        scores = jnp.sum(kbuf[b].astype(jnp.float32) * q_rows[rows_of(b), :][None], axis=-1, keepdims=True)
        scores = jnp.where(row_iota <= position, scores, -1e30)
        weights = jnp.exp(scores - jnp.max(scores, axis=0, keepdims=True))
        prob = weights * (1.0 / jnp.sum(weights, axis=0, keepdims=True))
        probs[b] = jnp.broadcast_to(prob, probs.shape[1:]).astype(jnp.bfloat16)

    def mix(b):
        vbuf[b, pos_ref[b]] = v_rows[rows_of(b), :].astype(jnp.bfloat16)
        mixed_rows[rows_of(b), :] = jnp.sum(probs[b].astype(jnp.float32) * vbuf[b].astype(jnp.float32), axis=0)

    def value_chunk(c):
        weight_copy(2 * chunks + c).wait()
        at = pl.ds(pl.multiple_of(c * cols, cols), cols)
        proj[2, :, at] = jnp.dot(normed, wbuf[2 * chunks + c], preferred_element_type=jnp.float32)

    trips = CACHE_BLOCKS * (block // SCORE_UNROLL)

    def sweep(kind, step, unroll):
        for i in range(CACHE_BLOCKS):
            cache_in(kind, i).wait()
            if kind == 0 and i == WO_AFTER:
                for index in range(3 * chunks, 4 * chunks):
                    weight_copy(index).start()

            def body(outer, carry):
                first = trips - chunks
                trip = i * (block // unroll)
                if kind == 0 and trip >= first:
                    value_chunk(trip - first + outer)
                for u in range(unroll):
                    step(i * block + outer * unroll + u)
                return carry

            lax.fori_loop(0, block // unroll, body, 0)
            if kind == 1:
                cache_out(0, i).start()
                cache_out(1, i).start()

    sweep(0, score, SCORE_UNROLL)
    for h in range(heads):
        v_rows[pl.ds(h, seqs, stride=heads), :] = proj[2, :, h * head_dim:(h + 1) * head_dim]
    sweep(1, mix, MIX_UNROLL)
    for h in range(heads):
        mixed[:, h * head_dim:(h + 1) * head_dim] = mixed_rows[pl.ds(h, seqs, stride=heads), :].astype(jnp.bfloat16)
    for c in range(chunks):
        if c % 2 == 0:
            weight_copy(3 * chunks + c).wait()
            weight_copy(3 * chunks + c + 1).wait()
        at = slice(c * cols, (c + 1) * cols)
        added = jnp.dot(mixed[...], wbuf[3 * chunks + c], preferred_element_type=jnp.float32)
        x_out[:, at] = (x_ref[:, at].astype(jnp.float32) + added).astype(jnp.bfloat16)
    result = pltpu.make_async_copy(x_out, x_hbm, x_sem)
    result.start()
    for i in range(CACHE_BLOCKS):
        for kind in range(2):
            cache_out(kind, i).wait()
    result.wait()


def attention_local(layer, hidden, positions, table, attn_gain, q_gain, k_gain, w_query, w_key, w_value, w_out, k_cache, v_cache, k_new, v_new):
    seqs, model = hidden.shape
    cache_shape = k_cache.shape[1:]
    heads, head_dim = cache_shape[2:]
    vmem = pl.BlockSpec(memory_space=pltpu.VMEM)
    smem = pl.BlockSpec(memory_space=pltpu.SMEM)
    hbm = pl.BlockSpec(memory_space=pl.ANY)
    operands = [positions, hidden, table, attn_gain, q_gain, k_gain, w_query, w_key, w_value, w_out, k_cache, v_cache]
    specs = [smem] + [vmem] * 5 + [hbm] * 6
    aliases = {}
    if k_new is not None:
        aliases = {len(operands): 1, len(operands) + 1: 2}
        operands += [k_new, v_new]
        specs += [hbm, hbm]
    chunks = model // COLS
    return pl.pallas_call(
        functools.partial(attention_kernel, layer, bool(aliases)),
        out_shape=(jax.ShapeDtypeStruct(hidden.shape, hidden.dtype), jax.ShapeDtypeStruct(k_cache.shape, k_cache.dtype), jax.ShapeDtypeStruct(v_cache.shape, v_cache.dtype)),
        in_specs=specs,
        out_specs=(hbm, hbm, hbm),
        input_output_aliases=aliases,
        scratch_shapes=[
            pltpu.VMEM(hidden.shape, hidden.dtype),
            pltpu.SemaphoreType.DMA,
            pltpu.VMEM((4 * chunks, model, COLS), jnp.bfloat16),
            pltpu.VMEM(cache_shape, jnp.bfloat16),
            pltpu.VMEM(cache_shape, jnp.bfloat16),
            pltpu.VMEM((3, seqs, model), jnp.float32),
            pltpu.VMEM((seqs * heads, head_dim), jnp.float32),
            pltpu.VMEM((seqs * heads, head_dim), jnp.float32),
            pltpu.VMEM((seqs * heads, head_dim), jnp.float32),
            pltpu.VMEM((seqs * heads, head_dim), jnp.float32),
            pltpu.VMEM((seqs, model), jnp.bfloat16),
            pltpu.VMEM(cache_shape, jnp.bfloat16),
            pltpu.VMEM((seqs, head_dim), jnp.float32),
            pltpu.VMEM((seqs, head_dim), jnp.float32),
            pltpu.SemaphoreType.DMA((4 * chunks,)),
            pltpu.SemaphoreType.DMA((2, CACHE_BLOCKS)),
            pltpu.SemaphoreType.DMA((2, CACHE_BLOCKS)),
        ],
        compiler_params=pltpu.CompilerParams(vmem_limit_bytes=67043328),
        name='attention_layer',
    )(*operands)


def moe_kernel(groups, layer, x_ref, routes_ref, gain_ref, wr_ref, wg, wu, wd, out_hbm, out_ref, out_sem, ring, rows, xg, act, ys, smat, meta, meta_in, part, dbuf, tbuf, f1, f2, ring_sem, down_sem, ag_send, ag_recv, meta_send, meta_recv, rs_send, rs_recv):
    seqs, model = x_ref.shape
    local_experts = wg.shape[0]
    experts = wr_ref.shape[0]
    ffn = wg.shape[2]
    slots = xg.shape[1] // groups
    chips = groups // 2
    me = lax.axis_index('ep')
    chip, core = me // 2, me % 2
    step = 1 - 2 * core
    partner = chip * 2 + 1 - core

    def device(offset, core_idx):
        return ((chip + offset + chips) % chips) * 2 + core_idx

    long_dev, short_dev, far_dev = device(step, core), device(-step, core), device(2 * step, core)
    gate_units = 2 * model // UNIT
    down_units = model // UNIT
    total_gate = gate_units * local_experts
    width = model // RS_CHUNKS
    per_unit = UNIT // width

    def gate_copy(expert, j):
        weights = wg if j < gate_units // 2 else wu
        slot = (expert * gate_units + j) % RING
        return pltpu.make_async_copy(weights.at[expert, pl.ds((j % (gate_units // 2)) * UNIT, UNIT), :], ring.at[slot], ring_sem.at[slot])

    def down_slot(unit):
        return (total_gate + unit) % RING

    def down_copy(unit, c):
        half, expert = unit // local_experts, unit % local_experts
        slot = down_slot(unit)
        return pltpu.make_async_copy(wd.at[expert, :, pl.ds(half * UNIT + c * width, width)], ring.at[slot, :, pl.ds(c * width, width)], down_sem.at[unit, c])

    ahead = RING // gate_units
    for expert in range(ahead):
        for j in range(gate_units):
            gate_copy(expert, j).start()

    barrier = pltpu.get_barrier_semaphore()
    for j in range(1, groups):
        pl.semaphore_signal(barrier, inc=1, device_id={'ep': (me + j) % groups}, device_id_type=MESH)

    values = x_ref[...].astype(jnp.float32)
    inv_rms = lax.rsqrt(jnp.mean(values * values, axis=-1, keepdims=True) + RMS_EPS)
    normed = (values * inv_rms * gain_ref[layer:layer + 1, :]).astype(jnp.bfloat16)
    rows[me] = normed
    pl.semaphore_wait(barrier, groups - 1)

    part_rows = seqs // AG_PARTS

    def rows_copy(role, source, peer, q):
        ref = rows.at[source, pl.ds(q * part_rows, part_rows), :]
        return pltpu.make_async_remote_copy(src_ref=ref, dst_ref=ref, send_sem=ag_send.at[role, q], recv_sem=ag_recv.at[role, q], device_id={'ep': peer}, device_id_type=MESH)

    plan = [(me, partner), (me, long_dev), (me, short_dev), (short_dev, long_dev), (short_dev, partner), (long_dev, partner), (far_dev, partner)]
    copies = [[rows_copy(role, source, peer, q) for q in range(AG_PARTS)] for role, (source, peer) in enumerate(plan)]
    for q in range(AG_PARTS):
        for role in (1, 2, 0):
            copies[role][q].start()

    logits = lax.dot_general(wr_ref[...], normed, (((1,), (1,)), ((), ())), preferred_element_type=jnp.float32)
    shifted = jnp.exp(logits - jnp.max(logits, axis=0, keepdims=True))
    prob = shifted / jnp.sum(shifted, axis=0, keepdims=True)
    expert_iota = lax.broadcasted_iota(jnp.int32, (experts, seqs), 0)
    routes = routes_ref[layer]
    chosen = expert_iota == routes[0:1, :]
    for j in range(1, routes.shape[0]):
        chosen = chosen | (expert_iota == routes[j:j + 1, :])
    row_iota = lax.broadcasted_iota(jnp.int32, (seqs, seqs), 0)
    col_iota = lax.broadcasted_iota(jnp.int32, (seqs, seqs), 1)
    upper = jnp.where(row_iota < col_iota, 1.0, 0.0).astype(jnp.bfloat16)
    ranks = jnp.dot(jnp.where(chosen, 1.0, 0.0).astype(jnp.bfloat16), upper, preferred_element_type=jnp.float32)
    fill = jnp.zeros((experts, LANES - seqs), jnp.float32)
    meta[:, :LANES] = jnp.concatenate([jnp.where(chosen, ranks, -1.0), fill - 1.0], axis=1)
    meta[:, LANES:] = jnp.concatenate([jnp.where(chosen, prob, 0.0), fill], axis=1)

    def meta_copy(j):
        peer = (me + j) % groups
        return pltpu.make_async_remote_copy(src_ref=meta.at[pl.ds(pl.multiple_of(peer * local_experts, local_experts), local_experts), :], dst_ref=meta_in.at[me], send_sem=meta_send.at[j], recv_sem=meta_recv.at[j], device_id={'ep': peer}, device_id_type=MESH)

    meta_copies = [meta_copy(j) for j in range(1, groups)]
    meta_in[me] = meta[pl.ds(pl.multiple_of(me * local_experts, local_experts), local_experts), :]
    for copy in meta_copies:
        copy.start()

    def gather(source):
        info = meta_in[source]
        rank = info[:, :LANES].reshape(local_experts, 1, LANES)
        gate = info[:, LANES:].reshape(local_experts, 1, LANES)
        place = lax.broadcasted_iota(jnp.int32, (local_experts, slots, LANES), 1).astype(jnp.float32)
        hit = jnp.broadcast_to(rank, place.shape) == place
        total = local_experts * slots
        onehot = jnp.where(hit, 1.0, 0.0).reshape(total, LANES)[:, :seqs].astype(jnp.bfloat16)
        taken = jnp.dot(onehot, rows[source], preferred_element_type=jnp.float32).astype(jnp.bfloat16)
        at = pl.ds(pl.multiple_of(source * slots, slots), slots)
        for e in range(local_experts):
            xg[e, at, :] = taken[e * slots:(e + 1) * slots]
        weight = jnp.where(hit, jnp.broadcast_to(gate, place.shape), 0.0).reshape(total, LANES).T[:seqs]
        first = weight.astype(jnp.bfloat16)
        rest = weight - first.astype(jnp.float32)
        second = rest.astype(jnp.bfloat16)
        third = (rest - second.astype(jnp.float32)).astype(jnp.bfloat16)
        smat[source, pl.ds(0, seqs), :] = first
        smat[source, pl.ds(seqs, seqs), :] = second
        smat[source, pl.ds(2 * seqs, seqs), :] = third

    gather(me)
    for q in range(AG_PARTS):
        copies[1][q].wait_recv()
        copies[3][q].start()
        copies[4][q].start()
        copies[2][q].wait_recv()
        copies[5][q].start()
    for copy in meta_copies:
        copy.wait_recv()
    for q in range(AG_PARTS):
        copies[0][q].wait_recv()
    gather(partner)
    gather(short_dev)
    gather(long_dev)
    for role in (4, 5):
        for q in range(AG_PARTS):
            copies[role][q].wait_recv()
    gather(device(step, 1 - core))
    gather(device(-step, 1 - core))
    for q in range(AG_PARTS):
        copies[3][q].wait_recv()
        copies[6][q].start()
    gather(far_dev)
    for q in range(AG_PARTS):
        copies[6][q].wait_recv()
    gather(device(2 * step, 1 - core))

    def expert_body(e, carry):
        for j in range(gate_units):
            gate_copy(e, j).wait()

        def product(first):
            total = None
            for j in range(gate_units // 2):
                slot = (e * gate_units + first + j) % RING
                term = jnp.dot(xg[e, :, pl.ds(j * UNIT, UNIT)], ring[slot], preferred_element_type=jnp.float32)
                total = term if total is None else total + term
            return total

        gate_act = product(0)
        up_act = product(gate_units // 2)
        act[e] = (jax.nn.silu(gate_act) * up_act).astype(jnp.bfloat16)

        @pl.when(e + ahead < local_experts)
        def _():
            for j in range(gate_units):
                gate_copy(e + ahead, j).start()

        for half in range(down_units):
            freed = (half + 1) * local_experts // gate_units + local_experts - ahead - 1

            @pl.when(e == freed)
            def _():
                for c in range(per_unit):
                    for expert in range(local_experts):
                        down_copy(half * local_experts + expert, c).start()

        return carry

    lax.fori_loop(0, local_experts, expert_body, 0)

    def rs_copy(role, k, source, target, peer):
        return pltpu.make_async_remote_copy(src_ref=source, dst_ref=target, send_sem=rs_send.at[role, k], recv_sem=rs_recv.at[role, k], device_id={'ep': peer}, device_id_type=MESH)

    far_chip, long_chip, short_chip = far_dev // 2, long_dev // 2, short_dev // 2

    def pair_copy(k):
        return rs_copy(0, k, part.at[k, 1 - core], dbuf.at[k], partner)

    def far_copy(k):
        return rs_copy(1, k, part.at[k, core, far_chip], tbuf.at[k], long_dev)

    def short_copy(k):
        return rs_copy(2, k, part.at[k, core, short_chip], f1.at[k], short_dev)

    def long_copy(k):
        return rs_copy(3, k, part.at[k, core, long_chip], f2.at[k], long_dev)

    def compute_chunk(k):
        half = k // per_unit
        column = (k % per_unit) * width

        units = [half * local_experts + e for e in range(local_experts)]
        for unit in units:
            down_copy(unit, k % per_unit).wait()
        for e, unit in enumerate(units):
            out = jnp.dot(act[e], ring[down_slot(unit), :, column:column + width], preferred_element_type=jnp.float32).astype(jnp.bfloat16)
            for b in range(groups):
                ys[b, e * slots:(e + 1) * slots, :] = out[b * slots:(b + 1) * slots]
        for b in range(groups):
            sums = jnp.dot(smat[b], ys[b], preferred_element_type=jnp.float32)
            part[k, b % 2, b // 2] = sums[:seqs] + sums[seqs:2 * seqs] + sums[2 * seqs:]

    def pair_sum(k):
        pair_copy(k).wait_recv()
        part[k, core] = part[k, core] + dbuf[k]
        far_copy(k).start()
        short_copy(k).start()

    def forward(k):
        far_copy(k).wait_recv()
        part[k, core, long_chip] = part[k, core, long_chip] + tbuf[k]
        long_copy(k).start()

    def finish(k):
        short_copy(k).wait_recv()
        long_copy(k).wait_recv()
        moe_out = part[k, core, chip] + f1[k] + f2[k]
        at = pl.ds(k * width, width)
        out_ref[:, at] = (x_ref[:, at].astype(jnp.float32) + moe_out).astype(jnp.bfloat16)

    for k in range(RS_CHUNKS):
        compute_chunk(k)
        pair_copy(k).start()
        if k >= 1:
            pair_sum(k - 1)
        if k >= FORWARD_LAG:
            forward(k - FORWARD_LAG)
    pair_sum(RS_CHUNKS - 1)
    for group in copies:
        for copy in group:
            copy.wait_send()
    for copy in meta_copies:
        copy.wait_send()
    for k in range(RS_CHUNKS - FORWARD_LAG):
        for make in (pair_copy, far_copy, short_copy):
            make(k).wait_send()
    for k in range(RS_CHUNKS - FORWARD_LAG, RS_CHUNKS):
        forward(k)
    for k in range(RS_CHUNKS):
        finish(k)
    result = pltpu.make_async_copy(out_ref, out_hbm, out_sem)
    result.start()
    for k in range(RS_CHUNKS):
        if k >= RS_CHUNKS - FORWARD_LAG:
            for make in (pair_copy, far_copy, short_copy):
                make(k).wait_send()
        long_copy(k).wait_send()
    result.wait()


def moe_local(hidden, routes, mlp_gain, w_router, w_gate, w_up, w_down, groups, layer):
    seqs, model = hidden.shape
    experts = w_router.shape[0]
    local_experts, _, ffn = w_gate.shape
    slots = CAP_FACTOR * seqs * routes.shape[1] // experts
    chips = groups // 2
    width = model // RS_CHUNKS
    vmem = pl.BlockSpec(memory_space=pltpu.VMEM)
    hbm = pl.BlockSpec(memory_space=pl.ANY)
    return pl.pallas_call(
        functools.partial(moe_kernel, groups, layer),
        out_shape=jax.ShapeDtypeStruct((seqs, model), jnp.bfloat16),
        in_specs=[vmem, vmem, vmem, vmem, hbm, hbm, hbm],
        out_specs=hbm,
        scratch_shapes=[
            pltpu.VMEM((seqs, model), jnp.bfloat16),
            pltpu.SemaphoreType.DMA,
            pltpu.VMEM((RING, UNIT, ffn), jnp.bfloat16),
            pltpu.VMEM((groups, seqs, model), jnp.bfloat16),
            pltpu.VMEM((local_experts, groups * slots, model), jnp.bfloat16),
            pltpu.VMEM((local_experts, groups * slots, ffn), jnp.bfloat16),
            pltpu.VMEM((groups, local_experts * slots, width), jnp.bfloat16),
            pltpu.VMEM((groups, 3 * seqs, local_experts * slots), jnp.bfloat16),
            pltpu.VMEM((experts, 2 * LANES), jnp.float32),
            pltpu.VMEM((groups, local_experts, 2 * LANES), jnp.float32),
            pltpu.VMEM((RS_CHUNKS, 2, chips, seqs, width), jnp.float32),
            pltpu.VMEM((RS_CHUNKS, chips, seqs, width), jnp.float32),
            pltpu.VMEM((RS_CHUNKS, seqs, width), jnp.float32),
            pltpu.VMEM((RS_CHUNKS, seqs, width), jnp.float32),
            pltpu.VMEM((RS_CHUNKS, seqs, width), jnp.float32),
            pltpu.SemaphoreType.DMA((RING,)),
            pltpu.SemaphoreType.DMA((model // UNIT * local_experts, UNIT // width)),
            pltpu.SemaphoreType.DMA((7, AG_PARTS)),
            pltpu.SemaphoreType.DMA((7, AG_PARTS)),
            pltpu.SemaphoreType.DMA((groups,)),
            pltpu.SemaphoreType.DMA((groups,)),
            pltpu.SemaphoreType.DMA((4, RS_CHUNKS)),
            pltpu.SemaphoreType.DMA((4, RS_CHUNKS)),
        ],
        compiler_params=pltpu.CompilerParams(collective_id=layer, has_side_effects=True, vmem_limit_bytes=67043328),
        name='moe_layer',
    )(hidden, routes, mlp_gain, w_router, w_gate, w_up, w_down)


def solution(mesh):
    groups = mesh.shape['ep']
    batch_axes = ('dp', 'ep')

    def device_step(hidden, positions, expert_ids, k_cache, v_cache, w_query, w_key, w_value, w_out, attn_gain, q_gain, k_gain, mlp_gain, w_router, w_gate, w_up, w_down):
        table = jnp.asarray(rope_table(k_cache.shape[2], k_cache.shape[4]))
        routes = jnp.swapaxes(expert_ids, 1, 2)
        router = w_router.T
        k_new, v_new = None, None
        for layer in range(expert_ids.shape[0]):
            hidden, k_new, v_new = attention_local(layer, hidden, positions, table, attn_gain, q_gain, k_gain, w_query, w_key, w_value, w_out, k_cache, v_cache, k_new, v_new)
            hidden = moe_local(hidden, routes, mlp_gain, router, w_gate, w_up, w_down, groups, layer)
        return hidden, k_new, v_new

    row_spec = P(batch_axes, None)
    cache_spec = P(None, batch_axes, None, None, None)
    full_spec = P()
    expert_spec = P('ep', None, None)
    in_specs = (row_spec, P(batch_axes), P(None, batch_axes, None), cache_spec, cache_spec, full_spec, full_spec, full_spec, full_spec, full_spec, full_spec, full_spec, full_spec, full_spec, expert_spec, expert_spec, expert_spec)
    return jax.shard_map(device_step, mesh=mesh, in_specs=in_specs, out_specs=(row_spec, cache_spec, cache_spec), check_vma=False)
```
